128 devices in a mesh: seq: 32 (over y, z, core), batch: 4 (over x).
Axes of the slice: x: 4, y: 4, z: 4, core: 2. Of those that a mesh axis runs over, the one named last changes fastest.
Arguments:
- queries: bfloat16 [4, 4096, 4096], P('batch', 'seq'), may hold values from -130 to 130
- keys: bfloat16 [4, 4096, 1024], P('batch', 'seq'), may hold values from -4 to 4
- values: bfloat16 [4, 4096, 1024], P('batch', 'seq'), may hold values from -4 to 4
- lengths: int32 [4], P('batch'), may hold values from 2048 to 4096
- block_pos: int32 [4, 32], P('batch'), may hold values from 0 to 31, each once within a row
- w_in: bfloat16 [6144, 1024], replicated, may hold values from -0.078125 to 0.078125
- b_in: float32 [1024], replicated, may hold values from -3 to 3
- output_weight: bfloat16 [1024, 8], replicated, may hold values from -0.1875 to 0.1875
- output_bias: float32 [8], replicated, may hold values from 1 to 2
Outputs:
- grad_w_in: float32 [6144, 1024], P(('seq', 'batch'))
- grad_b_in: float32 [1024], replicated
- output_weight_gradient: float32 [1024, 8], replicated
- output_bias_gradient: float32 [8], replicated
The draws below stay inside these ranges and needn't reach their ends.
Inputs may be any that keep to these rules, and one draw needn't show every extreme that they name: Each row of block_pos names every block 0 to 31 once.
All inputs are finite; a program needn't handle non-finite values.
Results may differ from the reference program's by a relative error of at most 0.0017.
The reference program's roundings to bfloat16 on the way (of `features`, `act`, `resid` and `delta`) count: a program that leaves them out, or rounds other values in their place, can miss the bound.
Values may be sent and summed in bfloat16 or wider, within the bound.
A program may use at most 128 MiB of HBM per device.

```python
import math
import jax
import jax.numpy as jnp
from jax import lax

QUERY_HEADS = 32
KEY_VALUE_HEADS = 8
HEAD_DIMENSION = 128
HIDDEN_UNITS = 1024
SEQ_DEV = 128
KD = 1024
FEAT = 6144
TOKEN_COUNT = 4096
SEQUENCE_COUNT = 4
N_SEQ = 32


def group_keys(key):
    base_offset = jax.random.fold_in(key, 7301)
    return jnp.clip(jax.random.normal(base_offset, (SEQUENCE_COUNT, TOKEN_COUNT, KEY_VALUE_HEADS * HEAD_DIMENSION), jnp.float32), -4.0, 4.0)


def draw_keys(key, part):
    base_offset = group_keys(key)
    return base_offset.astype(jnp.bfloat16)


def draw_queries(key, part):
    fresh = jax.random.fold_in(key, 1709)
    base_offset = jnp.clip(jax.random.normal(fresh, (SEQUENCE_COUNT, TOKEN_COUNT, QUERY_HEADS * HEAD_DIMENSION), jnp.float32), -4.0, 4.0)
    return base_offset.astype(jnp.bfloat16)


def place_ends(entries, stream_key, least, largest):
    index_at = [jax.random.randint(jax.random.fold_in(stream_key, axis), (), 0, length) for axis, length in enumerate(entries.shape)]
    widest = entries.shape.index(max(entries.shape))
    next_to = index_at[:widest] + [(index_at[widest] + 1) % entries.shape[widest]] + index_at[widest + 1:]
    return entries.at[tuple(index_at)].set(least).at[tuple(next_to)].set(largest)


def shard_levels(stream_key, shape, pieces, least, high):
    gain = 1.0
    for dim, blocks in pieces:
        steps = jax.random.uniform(jax.random.fold_in(jax.random.fold_in(stream_key, 6), dim), (blocks,), jnp.float32, least / len(pieces), high / len(pieces))
        gain = gain * jnp.repeat(jnp.exp(steps), shape[dim] // blocks).reshape((-1,) + (1,) * (len(shape) - 1 - dim))
    return gain


def bell_draw(stream_key, dims, scale, most, split=(), kind=jnp.bfloat16):
    array = jax.random.normal(stream_key, dims, jnp.float32) * scale
    if len(split) > 0:
        array = shard_levels(stream_key, dims, split, -0.22, 0.18) * array
    return jnp.clip(array, min=-most, max=most).astype(kind)


def setup_inputs(seed: int = 0) -> dict:
    seeds = jax.random.split(jax.random.key(seed), 10)
    queries = draw_queries(jax.random.fold_in(seeds[9], 71), 0)
    keys = draw_keys(jax.random.fold_in(seeds[9], 71), 0)
    values = bell_draw(seeds[2], (SEQUENCE_COUNT, TOKEN_COUNT, KD), 1.0, 4.0, ((0, 4), (1, 32)))
    lengths = place_ends(jax.random.randint(seeds[3], (SEQUENCE_COUNT,), TOKEN_COUNT // 2, TOKEN_COUNT + 1), jax.random.fold_in(seeds[3], 1), TOKEN_COUNT // 2, TOKEN_COUNT).astype(jnp.int32)
    block_pos = jax.vmap(lambda own: jax.random.permutation(own, N_SEQ))(jax.random.split(seeds[4], SEQUENCE_COUNT)).reshape((SEQUENCE_COUNT, N_SEQ)).astype(jnp.int32)
    w_in = bell_draw(seeds[5], (FEAT, HIDDEN_UNITS), FEAT ** -0.5, 0.078125)
    b_in = bell_draw(seeds[6], (HIDDEN_UNITS,), 0.5, 3.0, (), jnp.float32)
    output_weight = bell_draw(seeds[7], (HIDDEN_UNITS, KEY_VALUE_HEADS), HIDDEN_UNITS ** -0.5, 0.1875)
    output_bias = jnp.clip(jax.random.uniform(seeds[8], (KEY_VALUE_HEADS,), jnp.float32, 1.0, 2.0), 1.0, 2.0)
    return {"queries": queries, "keys": keys, "values": values, "lengths": lengths, "block_pos": block_pos, "w_in": w_in, "b_in": b_in, "output_weight": output_weight, "output_bias": output_bias}


def column_mass(q_rows, k_rows, positions, limit):
    group_index = QUERY_HEADS // KEY_VALUE_HEADS
    scale = 1.0 / math.sqrt(HEAD_DIMENSION)

    def queries_per_group(g, sums):
        g32 = jnp.asarray(g).astype(jnp.int32)
        k_part = lax.dynamic_slice_in_dim(k_rows, g32 * HEAD_DIMENSION, HEAD_DIMENSION, 1).astype(jnp.float32)
        key_live = positions < limit

        def per_block(i, column):
            i32 = jnp.asarray(i).astype(jnp.int32)
            start = i32 * SEQ_DEV
            q_part = lax.dynamic_slice(q_rows, (start, g32 * group_index * HEAD_DIMENSION), (SEQ_DEV, group_index * HEAD_DIMENSION))
            q_part = q_part.astype(jnp.float32).reshape(SEQ_DEV, group_index, HEAD_DIMENSION)
            q_pos = lax.dynamic_slice_in_dim(positions, start, SEQ_DEV)
            allowed = (positions[None, :] <= q_pos[:, None]) & key_live[None, :]
            scores = jnp.einsum('qhd,kd->hqk', q_part, k_part) * scale
            masked = jnp.where(allowed[None], scores, -1e+30)
            top = lax.optimization_barrier(jnp.max(masked, axis=2, keepdims=True))
            weights = jnp.where(allowed[None], jnp.exp(masked - top), 0.0)
            total = lax.optimization_barrier(jnp.sum(weights, axis=2, keepdims=True))
            q_live = (q_pos < limit).astype(jnp.float32)
            share = weights / total * q_live[None, :, None]
            return column + lax.optimization_barrier(jnp.sum(share, axis=(0, 1)))
        column = lax.fori_loop(0, N_SEQ, per_block, jnp.zeros((TOKEN_COUNT,), jnp.float32))
        return lax.dynamic_update_index_in_dim(sums, column, g32, 0)
    return lax.fori_loop(0, KEY_VALUE_HEADS, queries_per_group, jnp.zeros((KEY_VALUE_HEADS, TOKEN_COUNT), jnp.float32))

def reference(queries, keys, values, lengths, block_pos, w_in, b_in, output_weight, output_bias):
    norm = 1.0 / math.sqrt(SEQUENCE_COUNT * TOKEN_COUNT)
    offsets = jnp.arange(SEQ_DEV, dtype=jnp.int32)
    grad_w_in = jnp.zeros((FEAT, HIDDEN_UNITS), jnp.float32)
    grad_b_in = jnp.zeros((HIDDEN_UNITS,), jnp.float32)
    output_weight_gradient = jnp.zeros((HIDDEN_UNITS, KEY_VALUE_HEADS), jnp.float32)
    output_bias_gradient = jnp.zeros((KEY_VALUE_HEADS,), jnp.float32)
    for index in range(SEQUENCE_COUNT):
        q_rows = queries[index]
        k_rows = keys[index]
        v_rows = values[index]
        positions = (block_pos[index][:, None] * SEQ_DEV + offsets[None, :]).reshape(-1).astype(jnp.int32)
        limit = lengths[index]
        live = (positions < limit).astype(jnp.float32)
        mass = column_mass(q_rows, k_rows, positions, limit)
        labels = jnp.log1p(mass).T
        features = jnp.concatenate([q_rows, k_rows, v_rows], axis=1)
        pre = jnp.dot(features, w_in, preferred_element_type=jnp.float32) + b_in
        act = jax.nn.silu(pre).astype(jnp.bfloat16)
        pred = jnp.dot(act, output_weight, preferred_element_type=jnp.float32) + output_bias
        resid = ((pred - labels) * live[:, None] * norm).astype(jnp.bfloat16)
        back = jnp.dot(resid, output_weight.T, preferred_element_type=jnp.float32)
        sig = jax.nn.sigmoid(pre)
        delta = (back * sig * (1.0 + pre * (1.0 - sig))).astype(jnp.bfloat16)
        grad_w_in = grad_w_in + jnp.dot(features.T, delta, preferred_element_type=jnp.float32)
        grad_b_in = grad_b_in + lax.optimization_barrier(jnp.sum(delta.astype(jnp.float32), axis=0))
        output_weight_gradient = output_weight_gradient + jnp.dot(act.T, resid, preferred_element_type=jnp.float32)
        output_bias_gradient = output_bias_gradient + lax.optimization_barrier(jnp.sum(resid.astype(jnp.float32), axis=0))
    return (grad_w_in, grad_b_in, output_weight_gradient, output_bias_gradient)
```

```python
import functools
import math

import jax
import jax.numpy as jnp
from jax import lax
from jax.experimental import pallas as pl
from jax.experimental.pallas import tpu as pltpu
from jax.sharding import PartitionSpec as P

F32 = jnp.float32
BF16 = jnp.bfloat16
MESH = pl.DeviceIdType.MESH
SIDE = 4
ROUNDS = 2
GRAN = 16
LOG2E = 1.4426950408889634


def copy_to(src, dst, sems, index, target):
    return pltpu.make_async_remote_copy(
        src_ref=src,
        dst_ref=dst,
        send_sem=sems.at[(0, *index)],
        recv_sem=sems.at[(1, *index)],
        device_id=target,
        device_id_type=MESH,
    )


def kernel(
    n,
    nb,
    norm,
    scale,
    q_ref,
    k_ref,
    v_ref,
    w_ref,
    b_ref,
    wt_ref,
    bias_ref,
    order_ref,
    inv_ref,
    limit_ref,
    grad_ref,
    gb_ref,
    gw_ref,
    ob_ref,
    win,
    qg,
    kg,
    ks,
    qo,
    kt,
    ft,
    vt,
    slope,
    act,
    sref,
    colacc,
    mp,
    mr,
    dg,
    otc,
    otr,
    obs,
    obr,
    ofin,
    cs,
    cr,
    sb,
    xr,
    fin,
    fout,
    wsem,
    qsem,
    ksem,
    kpsem,
    qpsem,
    vsem,
    msem,
    asem,
    osem,
    bsem,
    hsem,
    psem,
    xsem,
    gsem,
):
    me = lax.axis_index("seq")
    mb = lax.axis_index("batch")
    rows, kd = k_ref.shape
    hidden = slope.shape[1]
    heads = wt_ref.shape[0] // 2
    head = kd // heads
    chips = n // 2
    chip = me // 2
    core = me % 2
    pair = chip * 2 + (1 - core)
    cy = chip // SIDE
    cz = chip % SIDE
    load = pltpu.make_async_copy(w_ref, win, wsem)
    load.start()

    def seq_peer(d):
        return lax.rem(me + d, n)

    def chip_peer(d):
        return lax.rem(chip + d, chips)

    def chip_source(d):
        return lax.rem(chip - d + chips, chips)

    def batch_peer(d):
        return lax.rem(mb + d, nb)

    def at(i, size):
        return pl.ds(pl.multiple_of(i * size, size), size)

    barrier = pltpu.get_barrier_semaphore()
    for d in range(1, n):
        pl.semaphore_signal(barrier, inc=1, device_id={"seq": seq_peer(d)}, device_id_type=MESH)
    for d in range(1, nb):
        pl.semaphore_signal(
            barrier, inc=1, device_id={"batch": batch_peer(d)}, device_id_type=MESH
        )

    def turn_values(j, carry):
        vt[at(j, head), :] = v_ref[:, at(j, head)].T
        return carry

    lax.fori_loop(0, kd // head, turn_values, 0)
    pl.semaphore_wait(barrier, n + nb - 2)

    key_far = []
    for d in range(1, chips):
        to = chip_peer(d)
        copy = copy_to(
            k_ref.at[:, at(to // 2, head)], kg.at[me], ksem, (d,), {"seq": to * 2 + core}
        )
        copy.start()
        key_far.append(copy)
    key_near = [
        copy_to(k_ref.at[:, at(chip // 2, head)], kg.at[me], kpsem, (0,), {"seq": pair})
    ]
    key_near[0].start()
    queries_sent = []
    for d in range(1, n):
        to = seq_peer(d)
        copy = copy_to(
            q_ref.at[:, at(to, head)], qg.at[me], qsem, (d,), {"seq": to}
        )
        copy.start()
        queries_sent.append(copy)
    vpart = kd // chips
    value_base = 2 * head + vpart
    values_sent = []
    for d in range(1, chips):
        to = chip_peer(d)
        copy = copy_to(
            vt.at[at(to, vpart)],
            ft.at[pl.ds(value_base, vpart), at(chip, rows)],
            vsem,
            (d,),
            {"seq": to * 2 + core},
        )
        copy.start()
        values_sent.append(copy)
    qg[me] = q_ref[:, at(me, head)]
    qo[at(chip, rows), :] = q_ref[:, at(pair, head)]
    kg[me] = k_ref[:, at(chip // 2, head)]
    ft[pl.ds(value_base, vpart), at(chip, rows)] = vt[at(chip, vpart), :]

    load.wait()
    tile = hidden // 4

    def project(j, carry):
        span = at(j, tile)
        value = b_ref[:, span]
        base = 0
        for ref in (q_ref, k_ref, v_ref):
            depth = ref.shape[1]
            value = value + jnp.dot(
                ref[...], win[base : base + depth, span], preferred_element_type=F32
            )
            base += depth
        sig = jax.nn.sigmoid(value)
        slope[:, span] = sig * (1.0 + value * (1.0 - sig))
        act[:, span] = (value * sig).astype(BF16)
        return carry

    lax.fori_loop(0, 4, project, 0)
    wt = wt_ref[...]
    pred = (
        lax.dot_general(wt, act[...], (((1,), (1,)), ((), ())), preferred_element_type=F32)[:heads]
        + bias_ref[...]
    )

    for d in range(1, chips):
        key_far[d - 1].wait_recv()
        held = kg.at[chip_source(d) * 2 + core]
        copy = copy_to(held, held, kpsem, (d,), {"seq": pair})
        copy.start()
        key_near.append(copy)
    for d in range(1, n):
        queries_sent[d - 1].wait_recv()
    queries_passed = []
    for d in range(1, chips):
        source = chip_source(d)
        copy = copy_to(
            qg.at[source * 2 + (1 - core)],
            qo.at[at(source, rows)],
            qpsem,
            (d,),
            {"seq": pair},
        )
        copy.start()
        queries_passed.append(copy)
    for copy in key_near:
        copy.wait_recv()

    limit = limit_ref[0]

    def sort_keys(p, carry):
        ks[at(p, rows), :] = kg[inv_ref[0, p]]
        return carry

    lax.fori_loop(0, n, sort_keys, 0)
    colacc[...] = jnp.zeros_like(colacc)
    step = 4
    wide = step * rows
    row_index = lax.broadcasted_iota(jnp.int32, (rows, 1), 0)
    lane_wide = lax.broadcasted_iota(jnp.int32, (1, wide), 1)

    for w in range(n // step):

        def query_block(t, carry, w=w):
            block = w * step + t
            queries = qg[inv_ref[0, block]]
            best = None
            for kc in range(w + 1):
                score = lax.dot_general(
                    queries,
                    ks[kc * wide : (kc + 1) * wide, :],
                    (((1,), (1,)), ((), ())),
                    preferred_element_type=F32,
                )
                if kc == w:
                    score = jnp.where(lane_wide <= row_index + t * rows, score, -1e30)
                sref[:, kc * wide : (kc + 1) * wide] = score
                for j in range(step):
                    part = score[:, j * rows : (j + 1) * rows]
                    best = part if best is None else jnp.maximum(best, part)
            top = jnp.max(best, axis=1, keepdims=True)
            total = None
            for kb in range((w + 1) * step):
                span = slice(kb * rows, (kb + 1) * rows)
                weight = jnp.exp2((sref[:, span] - top) * (scale * LOG2E))
                sref[:, span] = weight
                total = weight if total is None else total + weight
            denom = jnp.sum(total, axis=1, keepdims=True)
            live = (row_index + block * rows < limit).astype(F32)
            share = live / denom
            for kb in range((w + 1) * step):
                span = slice(kb * rows, (kb + 1) * rows)
                part = sref[:, span] * share
                colacc[kb] += jnp.sum(part.reshape(rows // 8, 8, rows), axis=0)
            return carry

        lax.fori_loop(0, step, query_block, 0)

    for t in range(n):
        mp[t] = colacc[order_ref[0, t]]
    mass_sent = []
    for d in range(1, n):
        to = seq_peer(d)
        copy = copy_to(mp.at[to], mr.at[me], msem, (d,), {"seq": to})
        copy.start()
        mass_sent.append(copy)
    mr[me] = mp[me]

    for copy in queries_passed:
        copy.wait_recv()
    for copy in values_sent:
        copy.wait_recv()

    def turn_features(s, carry):
        ft[at(core, head), at(s, rows)] = qg[2 * s + core].T
        ft[at(1 - core, head), at(s, rows)] = qo[at(s, rows), :].T
        kt[:, at(s, rows)] = kg[2 * s + core].T
        return carry

    lax.fori_loop(0, chips, turn_features, 0)
    ft[pl.ds(2 * head, vpart), :] = kt[at(chip % 2, vpart), :]

    for copy in mass_sent:
        copy.wait_recv()
    per_group = n // heads
    sums = []
    for g in range(heads):
        value = mr[g * per_group]
        for j in range(1, per_group):
            value = value + mr[g * per_group + j]
        sums.append(jnp.sum(value, axis=0, keepdims=True))
    mass = jnp.concatenate(sums, axis=0)
    lane = lax.broadcasted_iota(jnp.int32, (1, rows), 1)
    live_row = (lane + order_ref[0, me] * rows < limit).astype(F32)
    resid = ((pred - jnp.log1p(mass)) * live_row * norm).astype(BF16)
    resid32 = resid.astype(F32)
    resid_all = jnp.concatenate([resid32, jnp.zeros_like(resid32)], axis=0)
    back = jnp.dot(resid_all.T.astype(BF16), wt, preferred_element_type=F32)
    delta = (back * slope[...]).astype(BF16)
    blocks = hidden // rows
    for j in range(blocks):
        dg[j, at(chip, rows), :] = delta[:, j * rows : (j + 1) * rows]

    classes = blocks // ROUNDS
    gathered = {}

    def place(k, a, b):
        dy, dz = (a, b) if k < 2 else (b, a)
        return lax.rem(cy + SIDE - dy, SIDE) * SIDE + lax.rem(cz + SIDE - dz, SIDE)

    def forward(r, k, a, b, axis, move):
        along_y = (axis == 0) == (k < 2)
        if along_y:
            to = lax.rem(cy + SIDE + move, SIDE) * SIDE + cz
        else:
            to = cy * SIDE + lax.rem(cz + SIDE + move, SIDE)
        a2, b2 = ((a + move) % SIDE, b) if axis == 0 else (a, (b + move) % SIDE)
        part = dg.at[r * classes + k, at(place(k, a, b), rows)]
        copy = copy_to(part, part, asem, (r, k, a2 * SIDE + b2), {"seq": to * 2 + core})
        copy.start()
        gathered[r, k, a2, b2] = copy

    def arrive(r, k, a, b):
        gathered[r, k, a, b].wait_recv()

    def toward(k):
        return (1, 1, 3) if k % 2 == 0 else (-1, 3, 1)

    def stage0(r):
        for k in range(classes):
            for axis in (0, 1):
                for move in (1, -1):
                    forward(r, k, 0, 0, axis, move)

    def stage1(r):
        for k in range(classes):
            move, near, far = toward(k)
            arrive(r, k, near, 0)
            forward(r, k, near, 0, 0, move)
            forward(r, k, near, 0, 1, 1)
            forward(r, k, near, 0, 1, -1)
        for k in range(classes):
            move, near, far = toward(k)
            arrive(r, k, far, 0)
            forward(r, k, far, 0, 1, 1)
            forward(r, k, far, 0, 1, -1)

    def stage2(r):
        for k in range(classes):
            move, near, far = toward(k)
            arrive(r, k, 0, near)
            forward(r, k, 0, near, 1, move)
        for k in range(classes):
            arrive(r, k, 2, 0)
            forward(r, k, 2, 0, 1, 1)
            forward(r, k, 2, 0, 1, -1)

    def stage3(r):
        for a in (0, 1):
            for k in range(classes):
                move, near, far = toward(k)
                line = near if a == 0 else far
                arrive(r, k, line, near)
                forward(r, k, line, near, 1, move)

    def stage4(r):
        for k in range(classes):
            move, near, far = toward(k)
            arrive(r, k, 2, near)
            forward(r, k, 2, near, 1, move)

    def stage5(r):
        for k in range(classes):
            move, near, far = toward(k)
            for a in range(SIDE):
                arrive(r, k, a, far)
                arrive(r, k, a, 2)

    stage0(0)
    out_term = jnp.dot(resid_all.astype(BF16), act[...], preferred_element_type=F32)
    width = hidden // n
    bias_sum = jnp.broadcast_to(jnp.sum(resid32, axis=1, keepdims=True), (heads, width))
    delta_sum = jnp.sum(delta.astype(F32), axis=0, keepdims=True)
    for p in range(n):
        otc[p, :heads] = out_term[:heads, p * width : (p + 1) * width]
        otc[p, heads : 2 * heads] = bias_sum
        otc[p, 2 * heads :] = jnp.broadcast_to(
            delta_sum[:, p * width : (p + 1) * width], (heads, width)
        )
    stage1(0)
    stage0(1)
    first = []
    for d in range(1, n):
        to = seq_peer(d)
        copy = copy_to(otc.at[to], otr.at[d], osem, (d,), {"seq": to})
        copy.start()
        first.append(copy)
    stage2(0)
    stage3(0)
    stage1(1)
    small = otc[me]
    for d in range(1, n):
        first[d - 1].wait_recv()
        small = small + otr[d]
    obs[...] = small
    second = []
    for d in range(1, nb):
        copy = copy_to(obs, obr.at[d], bsem, (d,), {"batch": batch_peer(d)})
        copy.start()
        second.append(copy)
    stage4(0)
    stage2(1)
    stage5(0)

    half = ft.shape[0] // 2
    piece = hidden // ROUNDS
    share_rows = half // GRAN // nb

    def term(r, which):
        lhs = ft[at(which, half), :]
        parts = []
        for j in range(0, classes, 2):
            rhs = jnp.concatenate([dg[r * classes + j], dg[r * classes + j + 1]], axis=1)
            parts.append(jnp.dot(lhs, rhs, preferred_element_type=F32))
        return jnp.concatenate(parts, axis=1)

    def start_of(target):
        return lax.rem(share_rows * target + 2 * SIDE * chip, half // GRAN)

    swaps = []
    spread = []

    def swap(r):
        cs[r] = term(r, 1 - core)
        copy = copy_to(cs.at[r], cr.at[r], psem, (r,), {"seq": pair})
        copy.start()
        swaps.append(copy)

    def reduce_chip(r):
        own = term(r, core)
        swaps[r].wait_recv()
        both = (own + cr[r]).reshape(half // GRAN, GRAN, piece)
        sb[r, : half // GRAN] = both
        sb[r, half // GRAN :] = both[: share_rows - 1]
        for d in (2, 1, 3):
            to = batch_peer(d)
            copy = copy_to(
                sb.at[r, pl.ds(start_of(to), share_rows)],
                xr.at[r, d],
                xsem,
                (r, d),
                {"batch": to},
            )
            copy.start()
            spread.append((r, copy))

    def granule(i):
        q_gran = 2 * head // GRAN
        k_gran = vpart // GRAN
        total_q = n * head // GRAN
        total_k = kd // GRAN
        return jnp.where(
            i < q_gran,
            q_gran * chip + i,
            jnp.where(
                i < q_gran + k_gran,
                total_q + k_gran * chip + i - q_gran,
                total_q + total_k + k_gran * chip + i - q_gran - k_gran,
            ),
        )

    per_dev = share_rows * nb

    def owner_of(e):
        o = lax.rem(start_of(mb) + e, half // GRAN)
        return granule(o + core * (half // GRAN)) // per_dev

    def maker_of(e):
        q_gran = 2 * head // GRAN
        k_gran = vpart // GRAN
        total_q = n * head // GRAN
        total_k = kd // GRAN
        u = per_dev * me + share_rows * mb + e
        uk = u - total_q
        uv = uk - total_k
        which = jnp.where(
            uk < 0, u // q_gran, jnp.where(uv < 0, uk // k_gran, uv // k_gran)
        )
        i = jnp.where(
            uk < 0,
            u % q_gran,
            jnp.where(uv < 0, q_gran + uk % k_gran, q_gran + k_gran + uv % k_gran),
        )
        return which * 2 + jnp.where(i >= half // GRAN, 1, 0)

    def final_copy(r, e):
        return copy_to(fin.at[r, e], fout.at[r, e], gsem, (r, e), {"seq": owner_of(e)})

    def finish(r):
        value = sb[r, pl.ds(start_of(mb), share_rows)]
        for which, copy in spread:
            if which == r:
                copy.wait_recv()
        for d in range(1, nb):
            value = value + xr[r, d]
        fin[r] = value
        for e in range(share_rows):
            stays = owner_of(e) == me

            @pl.when(jnp.logical_not(stays))
            def _(r=r, e=e):
                final_copy(r, e).start()

            @pl.when(stays)
            def _(r=r, e=e):
                fout[r, e] = fin[r, e]

    swap(0)
    stage3(1)
    reduce_chip(0)
    stage4(1)
    small = obs[...]
    for d in range(1, nb):
        second[d - 1].wait_recv()
        small = small + obr[d]
    ofin[me] = small
    third = []
    for d in range(1, n):
        copy = copy_to(ofin.at[me], ofin.at[me], hsem, (d,), {"seq": seq_peer(d)})
        copy.start()
        third.append(copy)
    stage5(1)
    swap(1)
    finish(0)
    reduce_chip(1)
    for copy in third:
        copy.wait_recv()
    gw_ref[...] = jnp.concatenate([ofin[p, :heads] for p in range(n)], axis=1).T
    ob_ref[...] = ofin[0, heads : 2 * heads, :1]
    gb_ref[...] = jnp.concatenate([ofin[p, 2 * heads : 2 * heads + 1] for p in range(n)], axis=1)
    finish(1)
    for r in range(ROUNDS):
        for e in range(share_rows):

            @pl.when(maker_of(e) != me)
            def _(r=r, e=e):
                final_copy(r, e).wait_recv()

            grad_ref[e * GRAN : (e + 1) * GRAN, r * piece : (r + 1) * piece] = fout[r, e]
    for copy in (
        key_far
        + key_near
        + queries_sent
        + queries_passed
        + values_sent
        + mass_sent
        + list(gathered.values())
        + first
        + second
        + third
        + swaps
        + [copy for _, copy in spread]
    ):
        copy.wait_send()
    for r in range(ROUNDS):
        for e in range(share_rows):

            @pl.when(owner_of(e) != me)
            def _(r=r, e=e):
                final_copy(r, e).wait_send()


def on_device(queries, keys, values, lengths, block_pos, w_in, b_in, output_weight, output_bias):
    n = lax.axis_size("seq")
    nb = lax.axis_size("batch")
    q_rows = queries[0]
    k_rows = keys[0]
    v_rows = values[0]
    rows, kd = k_rows.shape
    heads = output_weight.shape[1]
    hidden = w_in.shape[1]
    feat = w_in.shape[0]
    head = kd // heads
    scale = 1.0 / math.sqrt(head)
    norm = 1.0 / math.sqrt(nb * n * rows)
    wt = jnp.pad(output_weight.T, ((0, heads), (0, 0)))
    vmem = pl.BlockSpec(memory_space=pltpu.VMEM)
    total = n * rows
    chips = n // 2
    part = feat // n // nb
    width = hidden // n
    chip_feat = feat // chips
    piece = hidden // ROUNDS
    grans = chip_feat // 2 // GRAN
    share_rows = grans // nb
    places = jnp.arange(n, dtype=jnp.int32)
    inverse = jnp.sum(
        jnp.where(block_pos[0][None, :] == places[:, None], places[None, :], 0), axis=1
    )[None, :]
    dma = pltpu.SemaphoreType.DMA
    grad, gb, gw, ob = pl.pallas_call(
        functools.partial(kernel, n, nb, norm, scale),
        out_shape=(
            jax.ShapeDtypeStruct((part, hidden), F32),
            jax.ShapeDtypeStruct((1, hidden), F32),
            jax.ShapeDtypeStruct((hidden, heads), F32),
            jax.ShapeDtypeStruct((heads, 1), F32),
        ),
        in_specs=[vmem] * 3
        + [pl.BlockSpec(memory_space=pl.ANY)]
        + [vmem] * 3
        + [pl.BlockSpec(memory_space=pltpu.SMEM)] * 3,
        out_specs=(vmem, vmem, vmem, vmem),
        scratch_shapes=[
            pltpu.VMEM((feat, hidden), BF16),
            pltpu.VMEM((n, rows, head), BF16),
            pltpu.VMEM((n, rows, head), BF16),
            pltpu.VMEM((total, head), BF16),
            pltpu.VMEM((total // 2, head), BF16),
            pltpu.VMEM((head, total // 2), BF16),
            pltpu.VMEM((chip_feat, total // 2), BF16),
            pltpu.VMEM((kd, rows), BF16),
            pltpu.VMEM((rows, hidden), F32),
            pltpu.VMEM((rows, hidden), BF16),
            pltpu.VMEM((rows, total), F32),
            pltpu.VMEM((n, 8, rows), F32),
            pltpu.VMEM((n, 8, rows), F32),
            pltpu.VMEM((n, 8, rows), F32),
            pltpu.VMEM((hidden // rows, total // 2, rows), BF16),
            pltpu.VMEM((n, 3 * heads, width), F32),
            pltpu.VMEM((n, 3 * heads, width), F32),
            pltpu.VMEM((3 * heads, width), F32),
            pltpu.VMEM((nb, 3 * heads, width), F32),
            pltpu.VMEM((n, 3 * heads, width), F32),
            pltpu.VMEM((ROUNDS, chip_feat // 2, piece), F32),
            pltpu.VMEM((ROUNDS, chip_feat // 2, piece), F32),
            pltpu.VMEM((ROUNDS, grans + share_rows - 1, GRAN, piece), F32),
            pltpu.VMEM((ROUNDS, nb, share_rows, GRAN, piece), F32),
            pltpu.VMEM((ROUNDS, share_rows, GRAN, piece), F32),
            pltpu.VMEM((ROUNDS, share_rows, GRAN, piece), F32),
            dma,
            dma((2, n)),
            dma((2, chips)),
            dma((2, chips)),
            dma((2, chips)),
            dma((2, chips)),
            dma((2, n)),
            dma((2, ROUNDS, hidden // rows // ROUNDS, SIDE * SIDE)),
            dma((2, n)),
            dma((2, nb)),
            dma((2, n)),
            dma((2, ROUNDS)),
            dma((2, ROUNDS, nb)),
            dma((2, ROUNDS, share_rows)),
        ],
        compiler_params=pltpu.CompilerParams(
            collective_id=0, has_side_effects=True, vmem_limit_bytes=60 * 1024 * 1024
        ),
    )(
        q_rows,
        k_rows,
        v_rows,
        w_in,
        b_in[None, :],
        wt,
        output_bias[:, None],
        block_pos,
        inverse,
        lengths,
    )
    return (grad, gb[0], gw, ob[:, 0])


def solution(mesh):
    return jax.shard_map(
        on_device,
        mesh=mesh,
        in_specs=(
            P("batch", "seq", None),
            P("batch", "seq", None),
            P("batch", "seq", None),
            P("batch"),
            P("batch", None),
            P(),
            P(),
            P(),
            P(),
        ),
        out_specs=(P(("seq", "batch"), None), P(), P(), P()),
        check_vma=False,
    )
```

```python
import functools
import math

import jax
import jax.numpy as jnp
from jax import lax
from jax.experimental import pallas as pl
from jax.experimental.pallas import tpu as pltpu
from jax.sharding import PartitionSpec as P

F32 = jnp.float32
BF16 = jnp.bfloat16
MESH = pl.DeviceIdType.MESH
SIDE = 4
ROUNDS = 2
FIXED = 54000.0
GRAN = 16
LOG2E = 1.4426950408889634


def copy_to(src, dst, sems, index, target):
    return pltpu.make_async_remote_copy(
        src_ref=src,
        dst_ref=dst,
        send_sem=sems.at[(0, *index)],
        recv_sem=sems.at[(1, *index)],
        device_id=target,
        device_id_type=MESH,
    )


def kernel(
    n,
    nb,
    norm,
    scale,
    q_ref,
    k_ref,
    v_ref,
    w_ref,
    b_ref,
    wt_ref,
    bias_ref,
    order_ref,
    limit_ref,
    grad_ref,
    small_ref,
    win,
    qg,
    kg,
    ks,
    qo,
    kt,
    ft,
    vt,
    slope,
    act,
    sref,
    colacc,
    mp,
    mr,
    predg,
    rs,
    dq,
    dg,
    otc,
    otr,
    obs,
    obr,
    ofin,
    cs,
    cr,
    sb,
    xr,
    fin,
    fout,
    inv,
    wsem,
    qsem,
    ksem,
    kpsem,
    qpsem,
    vsem,
    msem,
    dsem,
    asem,
    osem,
    bsem,
    hsem,
    psem,
    xsem,
    gsem,
):
    me = lax.axis_index("seq")
    mb = lax.axis_index("batch")
    rows, kd = k_ref.shape
    hidden = slope.shape[1]
    heads = wt_ref.shape[0]
    head = kd // heads
    chips = n // 2
    chip = me // 2
    core = me % 2
    pair = chip * 2 + (1 - core)
    cy = chip // SIDE
    cz = chip % SIDE
    load = pltpu.make_async_copy(w_ref, win, wsem)
    load.start()

    def seq_peer(d):
        return lax.rem(me + d, n)

    def chip_peer(d):
        return lax.rem(chip + d, chips)

    def chip_source(d):
        return lax.rem(chip - d + chips, chips)

    def batch_peer(d):
        return lax.rem(mb + d, nb)

    def at(i, size):
        return pl.ds(pl.multiple_of(i * size, size), size)

    barrier = pltpu.get_barrier_semaphore()
    for d in range(1, n):
        pl.semaphore_signal(barrier, inc=1, device_id={"seq": seq_peer(d)}, device_id_type=MESH)
    for d in range(1, nb):
        pl.semaphore_signal(
            barrier, inc=1, device_id={"batch": batch_peer(d)}, device_id_type=MESH
        )

    def turn_values(j, carry):
        vt[at(j, head), :] = v_ref[:, at(j, head)].T
        return carry

    lax.fori_loop(0, kd // head, turn_values, 0)
    pl.semaphore_wait(barrier, n + nb - 2)

    key_far = []
    for d in range(1, chips):
        to = chip_peer(d)
        copy = copy_to(
            k_ref.at[:, at(to // 2, head)], kg.at[me], ksem, (d,), {"seq": to * 2 + core}
        )
        copy.start()
        key_far.append(copy)
    key_near = [
        copy_to(k_ref.at[:, at(chip // 2, head)], kg.at[me], kpsem, (0,), {"seq": pair})
    ]
    key_near[0].start()
    queries_sent = []
    for d in range(1, n):
        to = seq_peer(d)
        copy = copy_to(
            q_ref.at[:, at(to, head)], qg.at[me], qsem, (d,), {"seq": to}
        )
        copy.start()
        queries_sent.append(copy)
    vpart = kd // chips
    value_base = 2 * head + vpart
    values_sent = []
    for d in range(1, chips):
        to = chip_peer(d)
        copy = copy_to(
            vt.at[at(to, vpart)],
            ft.at[pl.ds(value_base, vpart), at(chip, rows)],
            vsem,
            (d,),
            {"seq": to * 2 + core},
        )
        copy.start()
        values_sent.append(copy)
    qg[me] = q_ref[:, at(me, head)]
    qo[at(chip, rows), :] = q_ref[:, at(pair, head)]
    kg[me] = k_ref[:, at(chip // 2, head)]
    ft[pl.ds(value_base, vpart), at(chip, rows)] = vt[at(chip, vpart), :]

    def invert(p, carry):
        found = jnp.int32(0)
        for s in range(n):
            found = jnp.where(order_ref[0, s] == p, jnp.int32(s), found)
        inv[p] = found
        return carry

    lax.fori_loop(0, n, invert, 0)
    load.wait()
    tile = hidden // 4

    def project(j, carry):
        span = at(j, tile)
        value = b_ref[:, span]
        base = 0
        for ref in (q_ref, k_ref, v_ref):
            depth = ref.shape[1]
            value = value + jnp.dot(
                ref[...], win[base : base + depth, span], preferred_element_type=F32
            )
            base += depth
        sig = jax.nn.sigmoid(value)
        slope[:, span] = sig * (1.0 + value * (1.0 - sig))
        act[:, span] = (value * sig).astype(BF16)
        return carry

    lax.fori_loop(0, 4, project, 0)
    blocks = hidden // rows
    for j in range(blocks):
        fixed = jnp.floor((slope[:, j * rows : (j + 1) * rows] - 0.5) * FIXED + 0.5)
        dq[j, at(chip, rows), :] = fixed.astype(jnp.int32).astype(jnp.int16)

    classes = blocks // ROUNDS
    gathered = {}

    def place(k, a, b):
        dy, dz = (a, b) if k < 2 else (b, a)
        return lax.rem(cy + SIDE - dy, SIDE) * SIDE + lax.rem(cz + SIDE - dz, SIDE)

    def forward(r, k, a, b, axis, move):
        along_y = (axis == 0) == (k < 2)
        if along_y:
            to = lax.rem(cy + SIDE + move, SIDE) * SIDE + cz
        else:
            to = cy * SIDE + lax.rem(cz + SIDE + move, SIDE)
        a2, b2 = ((a + move) % SIDE, b) if axis == 0 else (a, (b + move) % SIDE)
        part = dq.at[r * classes + k, at(place(k, a, b), rows)]
        copy = copy_to(part, part, asem, (r, k, a2 * SIDE + b2), {"seq": to * 2 + core})
        copy.start()
        gathered[r, k, a2, b2] = copy

    def arrive(r, k, a, b):
        gathered[r, k, a, b].wait_recv()

    def toward(k):
        return (1, 1, 3) if k % 2 == 0 else (-1, 3, 1)

    def stage0(r):
        for k in range(classes):
            for axis in (0, 1):
                for move in (1, -1):
                    forward(r, k, 0, 0, axis, move)

    def stage1(r):
        for k in range(classes):
            move, near, far = toward(k)
            arrive(r, k, near, 0)
            forward(r, k, near, 0, 0, move)
            forward(r, k, near, 0, 1, 1)
            forward(r, k, near, 0, 1, -1)
        for k in range(classes):
            move, near, far = toward(k)
            arrive(r, k, far, 0)
            forward(r, k, far, 0, 1, 1)
            forward(r, k, far, 0, 1, -1)

    def stage2(r):
        for k in range(classes):
            move, near, far = toward(k)
            arrive(r, k, 0, near)
            forward(r, k, 0, near, 1, move)
        for k in range(classes):
            arrive(r, k, 2, 0)
            forward(r, k, 2, 0, 1, 1)
            forward(r, k, 2, 0, 1, -1)

    def stage3(r):
        for a in (0, 1):
            for k in range(classes):
                move, near, far = toward(k)
                line = near if a == 0 else far
                arrive(r, k, line, near)
                forward(r, k, line, near, 1, move)

    def stage4(r):
        for k in range(classes):
            move, near, far = toward(k)
            arrive(r, k, 2, near)
            forward(r, k, 2, near, 1, move)

    def stage5(r):
        for k in range(classes):
            move, near, far = toward(k)
            for a in range(SIDE):
                arrive(r, k, a, far)
                arrive(r, k, a, 2)

    stage0(0)
    stage0(1)
    wt32 = wt_ref[...].astype(F32)
    wt = jnp.concatenate([wt32, jnp.zeros_like(wt32)], axis=0).astype(BF16)
    group_index = lax.broadcasted_iota(jnp.int32, (heads, 1), 0)
    bias = jnp.zeros((heads, 1), F32)
    for g in range(heads):
        bias = jnp.where(group_index == g, bias_ref[0, g], bias)
    predg[chip] = (
        lax.dot_general(wt, act[...], (((1,), (1,)), ((), ())), preferred_element_type=F32)[:heads]
        + bias
    )
    preds_sent = []
    for d in range(1, chips):
        copy = copy_to(
            predg.at[chip], predg.at[chip], dsem, (d,), {"seq": chip_peer(d) * 2 + core}
        )
        copy.start()
        preds_sent.append(copy)

    for d in range(1, chips):
        key_far[d - 1].wait_recv()
        held = kg.at[chip_source(d) * 2 + core]
        copy = copy_to(held, held, kpsem, (d,), {"seq": pair})
        copy.start()
        key_near.append(copy)
    for d in range(1, n):
        queries_sent[d - 1].wait_recv()
    queries_passed = []
    for d in range(1, chips):
        source = chip_source(d)
        copy = copy_to(
            qg.at[source * 2 + (1 - core)],
            qo.at[at(source, rows)],
            qpsem,
            (d,),
            {"seq": pair},
        )
        copy.start()
        queries_passed.append(copy)
    for copy in key_near:
        copy.wait_recv()

    limit = limit_ref[0]

    def sort_keys(p, carry):
        ks[at(p, rows), :] = kg[inv[p]]
        return carry

    lax.fori_loop(0, n, sort_keys, 0)
    colacc[...] = jnp.zeros_like(colacc)
    step = 4
    wide = step * rows
    row_index = lax.broadcasted_iota(jnp.int32, (rows, 1), 0)
    lane_wide = lax.broadcasted_iota(jnp.int32, (1, wide), 1)

    for w in range(n // step):

        def query_block(t, carry, w=w):
            block = w * step + t
            queries = qg[inv[block]]
            best = None
            for kc in range(w + 1):
                score = lax.dot_general(
                    queries,
                    ks[kc * wide : (kc + 1) * wide, :],
                    (((1,), (1,)), ((), ())),
                    preferred_element_type=F32,
                )
                if kc == w:
                    score = jnp.where(lane_wide <= row_index + t * rows, score, -1e30)
                sref[:, kc * wide : (kc + 1) * wide] = score
                for j in range(step):
                    part = score[:, j * rows : (j + 1) * rows]
                    best = part if best is None else jnp.maximum(best, part)
            top = jnp.max(best, axis=1, keepdims=True)
            total = None
            for kb in range((w + 1) * step):
                span = slice(kb * rows, (kb + 1) * rows)
                weight = jnp.exp2((sref[:, span] - top) * (scale * LOG2E))
                sref[:, span] = weight
                total = weight if total is None else total + weight
            denom = jnp.sum(total, axis=1, keepdims=True)
            live = (row_index + block * rows < limit).astype(F32)
            share = live / denom
            for kb in range((w + 1) * step):
                span = slice(kb * rows, (kb + 1) * rows)
                part = sref[:, span] * share
                colacc[kb] += jnp.sum(part.reshape(rows // 8, 8, rows), axis=0)
            return carry

        lax.fori_loop(0, step, query_block, 0)
        if w == 2:
            stage1(0)
        elif w == 3:
            stage1(1)
        elif w == 4:
            stage2(0)
            stage3(0)
        elif w == 5:
            stage2(1)
            stage3(1)
        elif w == 6:
            stage4(0)
            stage4(1)

    for t in range(n):
        mp[t % 2, t // 2 : t // 2 + 1, :] = jnp.sum(
            colacc[order_ref[0, t]], axis=0, keepdims=True
        )
    mass_sent = []
    for d in range(1, n):
        to = seq_peer(d)
        copy = copy_to(mp.at[to % 2], mr.at[me], msem, (d,), {"seq": to})
        copy.start()
        mass_sent.append(copy)
    mr[me] = mp[core]

    for copy in queries_passed:
        copy.wait_recv()
    for copy in values_sent:
        copy.wait_recv()

    def turn_features(s, carry):
        ft[at(core, head), at(s, rows)] = qg[2 * s + core].T
        ft[at(1 - core, head), at(s, rows)] = qo[at(s, rows), :].T
        kt[:, at(s, rows)] = kg[2 * s + core].T
        return carry

    lax.fori_loop(0, chips, turn_features, 0)
    ft[pl.ds(2 * head, vpart), :] = kt[at(chip % 2, vpart), :]

    for copy in preds_sent:
        copy.wait_recv()
    for r in range(ROUNDS):
        stage5(r)
    for copy in mass_sent:
        copy.wait_recv()
    per_group = n // heads
    labels = []
    for g in range(heads):
        value = mr[g * per_group]
        for j in range(1, per_group):
            value = value + mr[g * per_group + j]
        labels.append(jnp.log1p(value))
    lane = lax.broadcasted_iota(jnp.int32, (1, rows), 1)
    for s in range(chips):
        label = jnp.concatenate([part[s : s + 1] for part in labels], axis=0)
        live_row = (lane + order_ref[0, 2 * s + core] * rows < limit).astype(F32)
        resid = ((predg[s] - label) * live_row * norm).astype(BF16).astype(F32)
        rs[s] = jnp.concatenate([resid, jnp.zeros_like(resid)], axis=0)

    def delta_round(r):
        base = r * classes

        def tokens(s, carry):
            back = jnp.dot(
                rs[s].T.astype(BF16),
                wt[:, base * rows : (base + classes) * rows],
                preferred_element_type=F32,
            )
            for j in range(classes):
                held = dq[base + j, at(s, rows), :].astype(jnp.int32).astype(F32)
                value = back[:, j * rows : (j + 1) * rows] * (held * (1.0 / FIXED) + 0.5)
                dg[base + j, at(s, rows), :] = value.astype(BF16)
            return carry

        lax.fori_loop(0, chips, tokens, 0)

    half = ft.shape[0] // 2
    piece = hidden // ROUNDS
    share_rows = half // GRAN // nb

    def term(r, which):
        lhs = ft[at(which, half), :]
        parts = []
        for j in range(0, classes, 2):
            rhs = jnp.concatenate([dg[r * classes + j], dg[r * classes + j + 1]], axis=1)
            parts.append(jnp.dot(lhs, rhs, preferred_element_type=F32))
        return jnp.concatenate(parts, axis=1)

    def start_of(target):
        return lax.rem(share_rows * target + 2 * SIDE * chip, half // GRAN)

    swaps = []
    spread = []

    def swap(r):
        cs[r] = term(r, 1 - core)
        copy = copy_to(cs.at[r], cr.at[r], psem, (r,), {"seq": pair})
        copy.start()
        swaps.append(copy)

    def reduce_chip(r):
        own = term(r, core)
        swaps[r].wait_recv()
        both = (own + cr[r]).reshape(half // GRAN, GRAN, piece)
        sb[r, : half // GRAN] = both
        sb[r, half // GRAN :] = both[: share_rows - 1]
        for d in (2, 1, 3):
            to = batch_peer(d)
            copy = copy_to(
                sb.at[r, pl.ds(start_of(to), share_rows)],
                xr.at[r, d],
                xsem,
                (r, d),
                {"batch": to},
            )
            copy.start()
            spread.append((r, copy))

    def granule(i):
        q_gran = 2 * head // GRAN
        k_gran = vpart // GRAN
        total_q = n * head // GRAN
        total_k = kd // GRAN
        return jnp.where(
            i < q_gran,
            q_gran * chip + i,
            jnp.where(
                i < q_gran + k_gran,
                total_q + k_gran * chip + i - q_gran,
                total_q + total_k + k_gran * chip + i - q_gran - k_gran,
            ),
        )

    per_dev = share_rows * nb

    def owner_of(e):
        o = lax.rem(start_of(mb) + e, half // GRAN)
        return granule(o + core * (half // GRAN)) // per_dev

    def maker_of(e):
        q_gran = 2 * head // GRAN
        k_gran = vpart // GRAN
        total_q = n * head // GRAN
        total_k = kd // GRAN
        u = per_dev * me + share_rows * mb + e
        uk = u - total_q
        uv = uk - total_k
        which = jnp.where(
            uk < 0, u // q_gran, jnp.where(uv < 0, uk // k_gran, uv // k_gran)
        )
        i = jnp.where(
            uk < 0,
            u % q_gran,
            jnp.where(uv < 0, q_gran + uk % k_gran, q_gran + k_gran + uv % k_gran),
        )
        return which * 2 + jnp.where(i >= half // GRAN, 1, 0)

    def final_copy(r, e):
        return copy_to(fin.at[r, e], fout.at[r, e], gsem, (r, e), {"seq": owner_of(e)})

    def finish(r):
        value = sb[r, pl.ds(start_of(mb), share_rows)]
        for which, copy in spread:
            if which == r:
                copy.wait_recv()
        for d in range(1, nb):
            value = value + xr[r, d]
        fin[r] = value
        for e in range(share_rows):
            stays = owner_of(e) == me

            @pl.when(jnp.logical_not(stays))
            def _(r=r, e=e):
                final_copy(r, e).start()

            @pl.when(stays)
            def _(r=r, e=e):
                fout[r, e] = fin[r, e]

    delta_round(0)
    swap(0)
    resid32 = rs[chip]
    out_term = jnp.dot(resid32.astype(BF16), act[...], preferred_element_type=F32)
    width = hidden // n
    bias_sum = jnp.broadcast_to(jnp.sum(resid32[:heads], axis=1, keepdims=True), (heads, width))
    delta = (
        jnp.dot(resid32.T.astype(BF16), wt, preferred_element_type=F32) * slope[...]
    ).astype(BF16)
    delta_sum = jnp.sum(delta.astype(F32), axis=0, keepdims=True)
    for p in range(n):
        otc[p, :heads] = out_term[:heads, p * width : (p + 1) * width]
        otc[p, heads : 2 * heads] = bias_sum
        otc[p, 2 * heads :] = jnp.broadcast_to(
            delta_sum[:, p * width : (p + 1) * width], (heads, width)
        )
    first = []
    for d in range(1, n):
        to = seq_peer(d)
        copy = copy_to(otc.at[to], otr.at[d], osem, (d,), {"seq": to})
        copy.start()
        first.append(copy)
    reduce_chip(0)
    delta_round(1)
    swap(1)
    small = otc[me]
    for d in range(1, n):
        first[d - 1].wait_recv()
        small = small + otr[d]
    obs[...] = small
    second = []
    for d in range(1, nb):
        copy = copy_to(obs, obr.at[d], bsem, (d,), {"batch": batch_peer(d)})
        copy.start()
        second.append(copy)
    reduce_chip(1)
    finish(0)
    small = obs[...]
    for d in range(1, nb):
        second[d - 1].wait_recv()
        small = small + obr[d]
    ofin[me] = small
    third = []
    for d in range(1, n):
        copy = copy_to(ofin.at[me], ofin.at[me], hsem, (d,), {"seq": seq_peer(d)})
        copy.start()
        third.append(copy)
    finish(1)
    for copy in third:
        copy.wait_recv()
    small_ref[:heads] = jnp.concatenate([ofin[p, :heads] for p in range(n)], axis=1)
    gb = jnp.concatenate([ofin[p, 2 * heads : 2 * heads + 1] for p in range(n)], axis=1)
    column = ofin[0, heads : 2 * heads, :1]
    lane_all = lax.broadcasted_iota(jnp.int32, (heads, hidden), 1)
    ob = jnp.sum(jnp.where(lane_all == group_index, column, 0.0), axis=0, keepdims=True)
    small_ref[heads:] = jnp.concatenate(
        [gb, ob, jnp.zeros((heads - 2, hidden), F32)], axis=0
    )
    for r in range(ROUNDS):
        for e in range(share_rows):

            @pl.when(maker_of(e) != me)
            def _(r=r, e=e):
                final_copy(r, e).wait_recv()

            grad_ref[e * GRAN : (e + 1) * GRAN, r * piece : (r + 1) * piece] = fout[r, e]
    for copy in (
        key_far
        + key_near
        + queries_sent
        + queries_passed
        + values_sent
        + mass_sent
        + preds_sent
        + list(gathered.values())
        + first
        + second
        + third
        + swaps
        + [copy for _, copy in spread]
    ):
        copy.wait_send()
    for r in range(ROUNDS):
        for e in range(share_rows):

            @pl.when(owner_of(e) != me)
            def _(r=r, e=e):
                final_copy(r, e).wait_send()


def emit(grad_in, small_in, grad_ref, gw_ref, gb_ref, ob_ref):
    heads = gw_ref.shape[0]
    grad_ref[...] = grad_in[...]
    gw_ref[...] = small_in[:heads]
    gb_ref[...] = small_in[heads : heads + 1]
    ob_ref[...] = small_in[heads + 1 : heads + 2, :heads]


def on_device(queries, keys, values, lengths, block_pos, w_in, b_in, output_weight, output_bias):
    n = lax.axis_size("seq")
    nb = lax.axis_size("batch")
    q_rows = queries[0]
    k_rows = keys[0]
    v_rows = values[0]
    rows, kd = k_rows.shape
    heads = output_weight.shape[1]
    hidden = w_in.shape[1]
    feat = w_in.shape[0]
    head = kd // heads
    scale = 1.0 / math.sqrt(head)
    norm = 1.0 / math.sqrt(nb * n * rows)
    vmem = pl.BlockSpec(memory_space=pltpu.VMEM)
    total = n * rows
    chips = n // 2
    part = feat // n // nb
    width = hidden // n
    chip_feat = feat // chips
    piece = hidden // ROUNDS
    grans = chip_feat // 2 // GRAN
    share_rows = grans // nb
    dma = pltpu.SemaphoreType.DMA
    grad, small = pl.pallas_call(
        functools.partial(kernel, n, nb, norm, scale),
        out_shape=(
            jax.ShapeDtypeStruct((part, hidden), F32),
            jax.ShapeDtypeStruct((2 * heads, hidden), F32),
        ),
        in_specs=[vmem] * 3
        + [pl.BlockSpec(memory_space=pl.ANY)]
        + [vmem] * 2
        + [pl.BlockSpec(memory_space=pltpu.SMEM)] * 3,
        out_specs=(vmem, vmem),
        scratch_shapes=[
            pltpu.VMEM((feat, hidden), BF16),
            pltpu.VMEM((n, rows, head), BF16),
            pltpu.VMEM((n, rows, head), BF16),
            pltpu.VMEM((total, head), BF16),
            pltpu.VMEM((total // 2, head), BF16),
            pltpu.VMEM((head, total // 2), BF16),
            pltpu.VMEM((chip_feat, total // 2), BF16),
            pltpu.VMEM((kd, rows), BF16),
            pltpu.VMEM((rows, hidden), F32),
            pltpu.VMEM((rows, hidden), BF16),
            pltpu.VMEM((rows, total), F32),
            pltpu.VMEM((n, 8, rows), F32),
            pltpu.VMEM((2, chips, rows), F32),
            pltpu.VMEM((n, chips, rows), F32),
            pltpu.VMEM((chips, heads, rows), F32),
            pltpu.VMEM((chips, 2 * heads, rows), F32),
            pltpu.VMEM((hidden // rows, total // 2, rows), jnp.int16),
            pltpu.VMEM((hidden // rows, total // 2, rows), BF16),
            pltpu.VMEM((n, 3 * heads, width), F32),
            pltpu.VMEM((n, 3 * heads, width), F32),
            pltpu.VMEM((3 * heads, width), F32),
            pltpu.VMEM((nb, 3 * heads, width), F32),
            pltpu.VMEM((n, 3 * heads, width), F32),
            pltpu.VMEM((ROUNDS, chip_feat // 2, piece), F32),
            pltpu.VMEM((ROUNDS, chip_feat // 2, piece), F32),
            pltpu.VMEM((ROUNDS, grans + share_rows - 1, GRAN, piece), F32),
            pltpu.VMEM((ROUNDS, nb, share_rows, GRAN, piece), F32),
            pltpu.VMEM((ROUNDS, share_rows, GRAN, piece), F32),
            pltpu.VMEM((ROUNDS, share_rows, GRAN, piece), F32),
            pltpu.SMEM((n,), jnp.int32),
            dma,
            dma((2, n)),
            dma((2, chips)),
            dma((2, chips)),
            dma((2, chips)),
            dma((2, chips)),
            dma((2, n)),
            dma((2, chips)),
            dma((2, ROUNDS, hidden // rows // ROUNDS, SIDE * SIDE)),
            dma((2, n)),
            dma((2, nb)),
            dma((2, n)),
            dma((2, ROUNDS)),
            dma((2, ROUNDS, nb)),
            dma((2, ROUNDS, share_rows)),
        ],
        compiler_params=pltpu.CompilerParams(
            collective_id=0, has_side_effects=True, vmem_limit_bytes=60 * 1024 * 1024
        ),
    )(
        q_rows,
        k_rows,
        v_rows,
        w_in,
        b_in[None, :],
        output_weight.T,
        output_bias[None, :],
        block_pos,
        lengths,
    )
    grad, gw, gb, ob = pl.pallas_call(
        emit,
        out_shape=(
            jax.ShapeDtypeStruct((part, hidden), F32),
            jax.ShapeDtypeStruct((heads, hidden), F32),
            jax.ShapeDtypeStruct((1, hidden), F32),
            jax.ShapeDtypeStruct((1, heads), F32),
        ),
        in_specs=[vmem] * 2,
        out_specs=(vmem,) * 4,
    )(grad, small)
    return (grad, gb[0], gw.T, ob[0])


def solution(mesh):
    return jax.shard_map(
        on_device,
        mesh=mesh,
        in_specs=(
            P("batch", "seq", None),
            P("batch", "seq", None),
            P("batch", "seq", None),
            P("batch"),
            P("batch", None),
            P(),
            P(),
            P(),
            P(),
        ),
        out_specs=(P(("seq", "batch"), None), P(), P(), P()),
        check_vma=False,
    )
```

```python
import functools
import math

import jax
import jax.numpy as jnp
from jax import lax
from jax.experimental import pallas as pl
from jax.experimental.pallas import tpu as pltpu
from jax.sharding import PartitionSpec as P

F32 = jnp.float32
BF16 = jnp.bfloat16
MESH = pl.DeviceIdType.MESH
SIDE = 4
ROUNDS = 2
CLASSES = 4
FIXED = 54000.0
GRAN = 16
LOG2E = 1.4426950408889634


def waiter(ref, sems, index):
    return pltpu.make_async_remote_copy(
        src_ref=ref,
        dst_ref=ref,
        send_sem=sems.at[(0, *index)],
        recv_sem=sems.at[(1, *index)],
        device_id={"seq": lax.axis_index("seq")},
        device_id_type=MESH,
    )


def copy_to(src, dst, sems, index, target):
    return pltpu.make_async_remote_copy(
        src_ref=src,
        dst_ref=dst,
        send_sem=sems.at[(0, *index)],
        recv_sem=sems.at[(1, *index)],
        device_id=target,
        device_id_type=MESH,
    )


def kernel(
    n,
    nb,
    norm,
    scale,
    q_ref,
    k_ref,
    v_ref,
    w_ref,
    b_ref,
    wt_ref,
    bias_ref,
    order_ref,
    limit_ref,
    grad_ref,
    small_ref,
    win,
    qg,
    kg,
    ks,
    qo,
    kt,
    ft,
    vt,
    slope,
    act,
    sref,
    colacc,
    mp,
    mr,
    predg,
    rs,
    dq,
    dg,
    otc,
    otr,
    obs,
    obr,
    ofin,
    cs,
    cr,
    sb,
    xr,
    fin,
    fout,
    inv,
    wsem,
    qsem,
    ksem,
    kpsem,
    qpsem,
    vsem,
    msem,
    dsem,
    asem,
    osem,
    bsem,
    hsem,
    psem,
    xsem,
    gsem,
):
    me = lax.axis_index("seq")
    mb = lax.axis_index("batch")
    rows, kd = k_ref.shape
    hidden = slope.shape[1]
    heads = wt_ref.shape[0]
    head = kd // heads
    chips = n // 2
    chip = me // 2
    core = me % 2
    pair = chip * 2 + (1 - core)
    cy = chip // SIDE
    cz = chip % SIDE
    load = pltpu.make_async_copy(w_ref, win, wsem)
    load.start()

    def seq_peer(d):
        return lax.rem(me + d, n)

    def chip_peer(d):
        return lax.rem(chip + d, chips)

    def chip_source(d):
        return lax.rem(chip - d + chips, chips)

    def batch_peer(d):
        return lax.rem(mb + d, nb)

    def at(i, size):
        return pl.ds(pl.multiple_of(i * size, size), size)

    barrier = pltpu.get_barrier_semaphore()
    for d in range(1, n):
        pl.semaphore_signal(barrier, inc=1, device_id={"seq": seq_peer(d)}, device_id_type=MESH)
    for d in range(1, nb):
        pl.semaphore_signal(
            barrier, inc=1, device_id={"batch": batch_peer(d)}, device_id_type=MESH
        )

    def turn_values(j, carry):
        vt[at(j, head), :] = v_ref[:, at(j, head)].T
        return carry

    lax.fori_loop(0, kd // head, turn_values, 0)
    pl.semaphore_wait(barrier, n + nb - 2)

    for d in range(1, chips):
        to = chip_peer(d)
        copy = copy_to(
            k_ref.at[:, at(to // 2, head)], kg.at[me], ksem, (), {"seq": to * 2 + core}
        )
        copy.start()
    copy_to(k_ref.at[:, at(chip // 2, head)], kg.at[me], kpsem, (), {"seq": pair}).start()
    for d in range(1, n):
        to = seq_peer(d)
        copy = copy_to(
            q_ref.at[:, at(to, head)], qg.at[me], qsem, (), {"seq": to}
        )
        copy.start()
    vpart = kd // chips
    value_base = 2 * head + vpart
    for d in range(1, chips):
        to = chip_peer(d)
        copy = copy_to(
            vt.at[at(to, vpart)],
            ft.at[pl.ds(value_base, vpart), at(chip, rows)],
            vsem,
            (),
            {"seq": to * 2 + core},
        )
        copy.start()
    qg[me] = q_ref[:, at(me, head)]
    qo[at(chip, rows), :] = q_ref[:, at(pair, head)]
    kg[me] = k_ref[:, at(chip // 2, head)]
    ft[pl.ds(value_base, vpart), at(chip, rows)] = vt[at(chip, vpart), :]

    def invert(p, carry):
        found = jnp.int32(0)
        for s in range(n):
            found = jnp.where(order_ref[0, s] == p, jnp.int32(s), found)
        inv[p] = found
        return carry

    lax.fori_loop(0, n, invert, 0)
    load.wait()
    tile = hidden // 4

    def project(j, carry):
        span = at(j, tile)
        value = b_ref[:, span]
        base = 0
        for ref in (q_ref, k_ref, v_ref):
            depth = ref.shape[1]
            value = value + jnp.dot(
                ref[...], win[base : base + depth, span], preferred_element_type=F32
            )
            base += depth
        sig = jax.nn.sigmoid(value)
        slope[:, span] = sig * (1.0 + value * (1.0 - sig))
        act[:, span] = (value * sig).astype(BF16)
        return carry

    lax.fori_loop(0, 4, project, 0)
    lanes = hidden // CLASSES
    for k in range(CLASSES):
        fixed = jnp.floor((slope[:, k * lanes : (k + 1) * lanes] - 0.5) * FIXED + 0.5)
        dq[k, at(chip, rows), :] = fixed.astype(jnp.int32).astype(jnp.int16)

    LAST = SIDE + 3

    def place(k, a, b):
        dy, dz = (a, b) if k < 2 else (b, a)
        return lax.rem(cy + SIDE - dy, SIDE) * SIDE + lax.rem(cz + SIDE - dz, SIDE)

    def toward(k):
        return (1, 1, 3) if k % 2 == 0 else (-1, 3, 1)

    def slot(k, a, b):
        move, near, far = toward(k)
        if b == 0:
            return a - 1
        return 3 + a if b == near else LAST

    def forward(k, a, b, axis, move):
        along_y = (axis == 0) == (k < 2)
        if along_y:
            to = lax.rem(cy + SIDE + move, SIDE) * SIDE + cz
        else:
            to = cy * SIDE + lax.rem(cz + SIDE + move, SIDE)
        a2, b2 = ((a + move) % SIDE, b) if axis == 0 else (a, (b + move) % SIDE)
        part = dq.at[k, at(place(k, a, b), rows)]
        pltpu.make_async_remote_copy(
            src_ref=part,
            dst_ref=part,
            send_sem=asem.at[CLASSES, 0],
            recv_sem=asem.at[k, slot(k, a2, b2)],
            device_id={"seq": to * 2 + core},
            device_id_type=MESH,
        ).start()

    def gathered(ref, k, i):
        return pltpu.make_async_remote_copy(
            src_ref=ref,
            dst_ref=ref,
            send_sem=asem.at[CLASSES, 0],
            recv_sem=asem.at[k, i],
            device_id={"seq": me},
            device_id_type=MESH,
        )

    def arrive(k, a, b):
        gathered(dq.at[k, at(place(k, a, b), rows)], k, slot(k, a, b)).wait_recv()

    def stage0():
        for axis in (0, 1):
            for k in range(CLASSES):
                for move in (1, -1):
                    forward(k, 0, 0, axis, move)

    def stage1():
        for k in range(CLASSES):
            move, near, far = toward(k)
            arrive(k, near, 0)
            forward(k, near, 0, 0, move)
            forward(k, near, 0, 1, 1)
            forward(k, near, 0, 1, -1)
        for k in range(CLASSES):
            move, near, far = toward(k)
            arrive(k, far, 0)
            forward(k, far, 0, 1, 1)
            forward(k, far, 0, 1, -1)

    def stage2():
        for k in range(CLASSES):
            move, near, far = toward(k)
            arrive(k, 0, near)
            forward(k, 0, near, 1, move)
        for k in range(CLASSES):
            arrive(k, 2, 0)
            forward(k, 2, 0, 1, 1)
            forward(k, 2, 0, 1, -1)

    def stage3():
        for a in (0, 1):
            for k in range(CLASSES):
                move, near, far = toward(k)
                line = near if a == 0 else far
                arrive(k, line, near)
                forward(k, line, near, 1, move)

    def stage4():
        for k in range(CLASSES):
            move, near, far = toward(k)
            arrive(k, 2, near)
            forward(k, 2, near, 1, move)

    def stage5():
        for k in range(CLASSES):
            gathered(dq.at[k, pl.ds(0, 2 * SIDE * rows)], k, LAST).wait_recv()

    stage0()
    wt32 = wt_ref[...].astype(F32)
    wt = jnp.concatenate([wt32, jnp.zeros_like(wt32)], axis=0).astype(BF16)
    group_index = lax.broadcasted_iota(jnp.int32, (heads, 1), 0)
    bias = jnp.zeros((heads, 1), F32)
    for g in range(heads):
        bias = jnp.where(group_index == g, bias_ref[0, g], bias)
    predg[chip] = (
        lax.dot_general(wt, act[...], (((1,), (1,)), ((), ())), preferred_element_type=F32)[:heads]
        + bias
    )
    for d in range(1, chips):
        copy = copy_to(
            predg.at[chip], predg.at[chip], dsem, (), {"seq": chip_peer(d) * 2 + core}
        )
        copy.start()

    waits = {
        "key_far": waiter(kg.at[pl.ds(0, chips - 1)], ksem, ()),
        "key_near": waiter(kg.at[pl.ds(0, chips)], kpsem, ()),
        "query": waiter(qg.at[pl.ds(0, n - 1)], qsem, ()),
        "query_near": waiter(qo.at[pl.ds(0, (chips - 1) * rows)], qpsem, ()),
        "value": waiter(
            ft.at[pl.ds(value_base, vpart), pl.ds(0, (chips - 1) * rows)], vsem, ()
        ),
        "mass": waiter(mr.at[pl.ds(0, n - 1)], msem, ()),
        "pred": waiter(predg.at[pl.ds(0, chips - 1)], dsem, ()),
    }
    waits["key_far"].wait_recv()
    for d in range(1, chips):
        held = kg.at[chip_source(d) * 2 + core]
        copy_to(held, held, kpsem, (), {"seq": pair}).start()
    waits["query"].wait_recv()
    for d in range(1, chips):
        source = chip_source(d)
        copy_to(
            qg.at[source * 2 + (1 - core)],
            qo.at[at(source, rows)],
            qpsem,
            (),
            {"seq": pair},
        ).start()
    waits["key_near"].wait_recv()

    limit = limit_ref[0]

    def sort_keys(p, carry):
        ks[at(p, rows), :] = kg[inv[p]]
        return carry

    lax.fori_loop(0, n, sort_keys, 0)
    colacc[...] = jnp.zeros_like(colacc)
    step = 4
    wide = step * rows
    row_index = lax.broadcasted_iota(jnp.int32, (rows, 1), 0)
    lane_wide = lax.broadcasted_iota(jnp.int32, (1, wide), 1)

    for w in range(n // step):

        def query_block(t, carry, w=w):
            block = w * step + t
            queries = qg[inv[block]]
            best = None
            for kc in range(w + 1):
                score = lax.dot_general(
                    queries,
                    ks[kc * wide : (kc + 1) * wide, :],
                    (((1,), (1,)), ((), ())),
                    preferred_element_type=F32,
                )
                if kc == w:
                    score = jnp.where(lane_wide <= row_index + t * rows, score, -1e30)
                sref[:, kc * wide : (kc + 1) * wide] = score
                for j in range(step):
                    part = score[:, j * rows : (j + 1) * rows]
                    best = part if best is None else jnp.maximum(best, part)
            top = jnp.max(best, axis=1, keepdims=True)
            total = None
            for kb in range((w + 1) * step):
                span = slice(kb * rows, (kb + 1) * rows)
                weight = jnp.exp2((sref[:, span] - top) * (scale * LOG2E))
                sref[:, span] = weight
                total = weight if total is None else total + weight
            denom = jnp.sum(total, axis=1, keepdims=True)
            live = (row_index + block * rows < limit).astype(F32)
            share = live / denom
            for kb in range((w + 1) * step):
                span = slice(kb * rows, (kb + 1) * rows)
                part = sref[:, span] * share
                colacc[kb] += jnp.sum(part.reshape(rows // 8, 8, rows), axis=0)
            return carry

        if w == n // step - 1:
            lax.fori_loop(0, step // 2, query_block, 0)
            stage4()
            lax.fori_loop(step // 2, step, query_block, 0)
        else:
            lax.fori_loop(0, step, query_block, 0)
        if w == 2:
            stage1()
        elif w == 4:
            stage2()
        elif w == 6:
            stage3()

    for t in range(n):
        mp[t % 2, t // 2 : t // 2 + 1, :] = jnp.sum(
            colacc[order_ref[0, t]], axis=0, keepdims=True
        )
    for d in range(1, n):
        to = seq_peer(d)
        copy_to(mp.at[to % 2], mr.at[me], msem, (), {"seq": to}).start()
    mr[me] = mp[core]

    waits["query_near"].wait_recv()
    waits["value"].wait_recv()

    def turn_features(s, carry):
        ft[at(core, head), at(s, rows)] = qg[2 * s + core].T
        ft[at(1 - core, head), at(s, rows)] = qo[at(s, rows), :].T
        kt[:, at(s, rows)] = kg[2 * s + core].T
        return carry

    lax.fori_loop(0, chips, turn_features, 0)
    ft[pl.ds(2 * head, vpart), :] = kt[at(chip % 2, vpart), :]

    waits["pred"].wait_recv()
    waits["mass"].wait_recv()
    per_group = n // heads
    labels = []
    for g in range(heads):
        value = mr[g * per_group]
        for j in range(1, per_group):
            value = value + mr[g * per_group + j]
        labels.append(jnp.log1p(value))
    lane = lax.broadcasted_iota(jnp.int32, (1, rows), 1)
    for s in range(chips):
        label = jnp.concatenate([part[s : s + 1] for part in labels], axis=0)
        live_row = (lane + order_ref[0, 2 * s + core] * rows < limit).astype(F32)
        resid = ((predg[s] - label) * live_row * norm).astype(BF16).astype(F32)
        rs[s] = jnp.concatenate([resid, jnp.zeros_like(resid)], axis=0)

    per_round = CLASSES // ROUNDS

    def delta_round(r):
        base = r * per_round

        def tokens(s, carry):
            back = jnp.dot(
                rs[s].T.astype(BF16),
                wt[:, base * lanes : (base + per_round) * lanes],
                preferred_element_type=F32,
            )
            for j in range(per_round):
                held = dq[base + j, at(s, rows), :].astype(jnp.int32).astype(F32)
                value = back[:, j * lanes : (j + 1) * lanes] * (held * (1.0 / FIXED) + 0.5)
                dg[base + j, at(s, rows), :] = value.astype(BF16)
            return carry

        lax.fori_loop(0, chips, tokens, 0)

    half = ft.shape[0] // 2
    piece = hidden // ROUNDS
    share_rows = half // GRAN // nb

    def term(r, which):
        lhs = ft[at(which, half), :]
        parts = [
            jnp.dot(lhs, dg[r * per_round + j], preferred_element_type=F32)
            for j in range(per_round)
        ]
        return jnp.concatenate(parts, axis=1)

    def start_of(target):
        return lax.rem(share_rows * target + 2 * SIDE * chip, half // GRAN)

    swaps = []

    def swap(r):
        cs[r] = term(r, 1 - core)
        copy = copy_to(cs.at[r], cr.at[r], psem, (r,), {"seq": pair})
        copy.start()
        swaps.append(copy)

    def reduce_chip(r):
        own = term(r, core)
        swaps[r].wait_recv()
        both = (own + cr[r]).reshape(half // GRAN, GRAN, piece)
        sb[r, : half // GRAN] = both
        sb[r, half // GRAN :] = both[: share_rows - 1]
        for d in (2, 1, 3):
            to = batch_peer(d)
            copy = copy_to(
                sb.at[r, pl.ds(start_of(to), share_rows)],
                xr.at[r, d - 1],
                xsem,
                (r,),
                {"batch": to},
            )
            copy.start()

    def granule(i):
        q_gran = 2 * head // GRAN
        k_gran = vpart // GRAN
        total_q = n * head // GRAN
        total_k = kd // GRAN
        return jnp.where(
            i < q_gran,
            q_gran * chip + i,
            jnp.where(
                i < q_gran + k_gran,
                total_q + k_gran * chip + i - q_gran,
                total_q + total_k + k_gran * chip + i - q_gran - k_gran,
            ),
        )

    per_dev = share_rows * nb

    def owner_of(e):
        o = lax.rem(start_of(mb) + e, half // GRAN)
        return granule(o + core * (half // GRAN)) // per_dev

    def maker_of(e):
        q_gran = 2 * head // GRAN
        k_gran = vpart // GRAN
        total_q = n * head // GRAN
        total_k = kd // GRAN
        u = per_dev * me + share_rows * mb + e
        uk = u - total_q
        uv = uk - total_k
        which = jnp.where(
            uk < 0, u // q_gran, jnp.where(uv < 0, uk // k_gran, uv // k_gran)
        )
        i = jnp.where(
            uk < 0,
            u % q_gran,
            jnp.where(uv < 0, q_gran + uk % k_gran, q_gran + k_gran + uv % k_gran),
        )
        return which * 2 + jnp.where(i >= half // GRAN, 1, 0)

    def final_copy(r, e):
        return copy_to(fin.at[r, e], fout.at[r, e], gsem, (r, e), {"seq": owner_of(e)})

    def finish(r):
        value = sb[r, pl.ds(start_of(mb), share_rows)]
        waiter(xr.at[r], xsem, (r,)).wait_recv()
        for d in range(nb - 1):
            value = value + xr[r, d]
        fin[r] = value
        for e in range(share_rows):
            stays = owner_of(e) == me

            @pl.when(jnp.logical_not(stays))
            def _(r=r, e=e):
                final_copy(r, e).start()

            @pl.when(stays)
            def _(r=r, e=e):
                fout[r, e] = fin[r, e]

    every = n // otc.shape[0]
    pieces = otc.shape[0]
    reduces = lax.rem(me, every) == 0
    resid32 = rs[chip]
    out_term = jnp.dot(resid32.astype(BF16), act[...], preferred_element_type=F32)[:heads]
    lane_row = lax.broadcasted_iota(jnp.int32, (heads, rows), 1)
    bias_row = jnp.sum(
        jnp.where(
            lane_row == group_index, jnp.sum(resid32[:heads], axis=1, keepdims=True), 0.0
        ),
        axis=0,
        keepdims=True,
    )
    delta = (
        jnp.dot(resid32.T.astype(BF16), wt, preferred_element_type=F32) * slope[...]
    ).astype(BF16)
    delta_sum = jnp.sum(delta.astype(F32), axis=0, keepdims=True)
    filler = jnp.zeros((heads - 2, rows), F32)
    for p in range(pieces):
        span = slice(p * rows, (p + 1) * rows)
        otc[p] = jnp.concatenate([out_term[:, span], delta_sum[:, span], bias_row, filler], axis=0)

    def small_copy(p):
        return copy_to(otc.at[p], otr.at[me], osem, (), {"seq": jnp.int32(p * every)})

    for p in range(pieces):

        @pl.when(me != p * every)
        def _(p=p):
            small_copy(p).start()

    stage5()
    delta_round(0)
    swap(0)

    @pl.when(reduces)
    def _():
        otr[me] = otc[me // every]
        waiter(otr.at[pl.ds(0, n - 1)], osem, ()).wait_recv()
        total = otr[0]
        for d in range(1, n):
            total = total + otr[d]
        obs[...] = total
        for d in range(1, nb):
            copy_to(obs, obr.at[d - 1], bsem, (), {"batch": batch_peer(d)}).start()

    reduce_chip(0)
    delta_round(1)
    swap(1)

    @pl.when(reduces)
    def _():
        waiter(obr, bsem, ()).wait_recv()
        total = obs[...]
        for d in range(nb - 1):
            total = total + obr[d]
        ofin[me // every] = total
        done = ofin.at[me // every]
        for d in range(1, n):
            copy_to(done, done, hsem, (), {"seq": seq_peer(d)}).start()

    reduce_chip(1)
    finish(0)
    finish(1)

    @pl.when(reduces)
    def _():
        waiter(ofin.at[pl.ds(0, pieces - 1)], hsem, ()).wait_recv()

    @pl.when(jnp.logical_not(reduces))
    def _():
        waiter(ofin, hsem, ()).wait_recv()

    small = jnp.concatenate([ofin[p] for p in range(pieces)], axis=1)
    small_ref[...] = small
    for r in range(ROUNDS):
        for e in range(share_rows):

            @pl.when(maker_of(e) != me)
            def _(r=r, e=e):
                final_copy(r, e).wait_recv()

            grad_ref[e * GRAN : (e + 1) * GRAN, r * piece : (r + 1) * piece] = fout[r, e]
    for wait in waits.values():
        wait.wait_send()
    gathered(dq.at[:, pl.ds(0, (SIDE * SIDE - 1) * rows)], 0, 0).wait_send()

    @pl.when(reduces)
    def _():
        waiter(otc.at[pl.ds(0, pieces - 1)], osem, ()).wait_send()
        waiter(obr, bsem, ()).wait_send()
        waiter(otr.at[pl.ds(0, n - 1)], hsem, ()).wait_send()

    @pl.when(jnp.logical_not(reduces))
    def _():
        waiter(otc, osem, ()).wait_send()

    for r in range(ROUNDS):
        swaps[r].wait_send()
        waiter(xr.at[r], xsem, (r,)).wait_send()
    for r in range(ROUNDS):
        for e in range(share_rows):

            @pl.when(owner_of(e) != me)
            def _(r=r, e=e):
                final_copy(r, e).wait_send()


def emit(grad_in, small_in, grad_ref, gw_ref, gb_ref, ob_ref):
    heads = gw_ref.shape[0]
    grad_ref[...] = grad_in[...]
    gw_ref[...] = small_in[:heads]
    gb_ref[...] = small_in[heads : heads + 1]
    ob_ref[...] = small_in[heads + 1 : heads + 2, :heads]


def on_device(queries, keys, values, lengths, block_pos, w_in, b_in, output_weight, output_bias):
    n = lax.axis_size("seq")
    nb = lax.axis_size("batch")
    q_rows = queries[0]
    k_rows = keys[0]
    v_rows = values[0]
    rows, kd = k_rows.shape
    heads = output_weight.shape[1]
    hidden = w_in.shape[1]
    feat = w_in.shape[0]
    head = kd // heads
    scale = 1.0 / math.sqrt(head)
    norm = 1.0 / math.sqrt(nb * n * rows)
    vmem = pl.BlockSpec(memory_space=pltpu.VMEM)
    total = n * rows
    chips = n // 2
    part = feat // n // nb
    chip_feat = feat // chips
    piece = hidden // ROUNDS
    grans = chip_feat // 2 // GRAN
    share_rows = grans // nb
    dma = pltpu.SemaphoreType.DMA
    grad, small = pl.pallas_call(
        functools.partial(kernel, n, nb, norm, scale),
        out_shape=(
            jax.ShapeDtypeStruct((part, hidden), F32),
            jax.ShapeDtypeStruct((2 * heads, hidden), F32),
        ),
        in_specs=[vmem] * 3
        + [pl.BlockSpec(memory_space=pl.ANY)]
        + [vmem] * 2
        + [pl.BlockSpec(memory_space=pltpu.SMEM)] * 3,
        out_specs=(vmem, vmem),
        scratch_shapes=[
            pltpu.VMEM((feat, hidden), BF16),
            pltpu.VMEM((n, rows, head), BF16),
            pltpu.VMEM((n, rows, head), BF16),
            pltpu.VMEM((total, head), BF16),
            pltpu.VMEM((total // 2, head), BF16),
            pltpu.VMEM((head, total // 2), BF16),
            pltpu.VMEM((chip_feat, total // 2), BF16),
            pltpu.VMEM((kd, rows), BF16),
            pltpu.VMEM((rows, hidden), F32),
            pltpu.VMEM((rows, hidden), BF16),
            pltpu.VMEM((rows, total), F32),
            pltpu.VMEM((n, 8, rows), F32),
            pltpu.VMEM((2, chips, rows), F32),
            pltpu.VMEM((n, chips, rows), F32),
            pltpu.VMEM((chips, heads, rows), F32),
            pltpu.VMEM((chips, 2 * heads, rows), F32),
            pltpu.VMEM((CLASSES, total // 2, hidden // CLASSES), jnp.int16),
            pltpu.VMEM((CLASSES, total // 2, hidden // CLASSES), BF16),
            pltpu.VMEM((hidden // rows, 2 * heads, rows), F32),
            pltpu.VMEM((n, 2 * heads, rows), F32),
            pltpu.VMEM((2 * heads, rows), F32),
            pltpu.VMEM((nb - 1, 2 * heads, rows), F32),
            pltpu.VMEM((hidden // rows, 2 * heads, rows), F32),
            pltpu.VMEM((ROUNDS, chip_feat // 2, piece), F32),
            pltpu.VMEM((ROUNDS, chip_feat // 2, piece), F32),
            pltpu.VMEM((ROUNDS, grans + share_rows - 1, GRAN, piece), F32),
            pltpu.VMEM((ROUNDS, nb - 1, share_rows, GRAN, piece), F32),
            pltpu.VMEM((ROUNDS, share_rows, GRAN, piece), F32),
            pltpu.VMEM((ROUNDS, share_rows, GRAN, piece), F32),
            pltpu.SMEM((n,), jnp.int32),
            dma,
            dma((2,)),
            dma((2,)),
            dma((2,)),
            dma((2,)),
            dma((2,)),
            dma((2,)),
            dma((2,)),
            dma((CLASSES + 1, SIDE + 4)),
            dma((2,)),
            dma((2,)),
            dma((2,)),
            dma((2, ROUNDS)),
            dma((2, ROUNDS)),
            dma((2, ROUNDS, share_rows)),
        ],
        compiler_params=pltpu.CompilerParams(
            collective_id=0, has_side_effects=True, vmem_limit_bytes=60 * 1024 * 1024
        ),
    )(
        q_rows,
        k_rows,
        v_rows,
        w_in,
        b_in[None, :],
        output_weight.T,
        output_bias[None, :],
        block_pos,
        lengths,
    )
    grad, gw, gb, ob = pl.pallas_call(
        emit,
        out_shape=(
            jax.ShapeDtypeStruct((part, hidden), F32),
            jax.ShapeDtypeStruct((heads, hidden), F32),
            jax.ShapeDtypeStruct((1, hidden), F32),
            jax.ShapeDtypeStruct((1, heads), F32),
        ),
        in_specs=[vmem] * 2,
        out_specs=(vmem,) * 4,
    )(grad, small)
    return (grad, gb[0], gw.T, ob[0])


def solution(mesh):
    return jax.shard_map(
        on_device,
        mesh=mesh,
        in_specs=(
            P("batch", "seq", None),
            P("batch", "seq", None),
            P("batch", "seq", None),
            P("batch"),
            P("batch", None),
            P(),
            P(),
            P(),
            P(),
        ),
        out_specs=(P(("seq", "batch"), None), P(), P(), P()),
        check_vma=False,
    )
```

```python
import functools
import math

import jax
import jax.numpy as jnp
from jax import lax
from jax.experimental import pallas as pl
from jax.experimental.pallas import tpu as pltpu
from jax.sharding import PartitionSpec as P

F32 = jnp.float32
BF16 = jnp.bfloat16
MESH = pl.DeviceIdType.MESH
SIDE = 4
ROUNDS = 4
CLASSES = 4
FIXED = 54000.0
GRAN = 16
LOG2E = 1.4426950408889634


def waiter(ref, sems, index):
    return pltpu.make_async_remote_copy(
        src_ref=ref,
        dst_ref=ref,
        send_sem=sems.at[(0, *index)],
        recv_sem=sems.at[(1, *index)],
        device_id={"seq": lax.axis_index("seq")},
        device_id_type=MESH,
    )


def copy_to(src, dst, sems, index, target):
    return pltpu.make_async_remote_copy(
        src_ref=src,
        dst_ref=dst,
        send_sem=sems.at[(0, *index)],
        recv_sem=sems.at[(1, *index)],
        device_id=target,
        device_id_type=MESH,
    )


def kernel(
    n,
    nb,
    norm,
    scale,
    q_ref,
    k_ref,
    v_ref,
    w_ref,
    b_ref,
    wt_ref,
    bias_ref,
    order_ref,
    limit_ref,
    grad_ref,
    small_ref,
    win,
    qg,
    kg,
    ks,
    qo,
    kt,
    ft,
    vt,
    slope,
    act,
    sref,
    colacc,
    mp,
    mr,
    predg,
    rs,
    rt,
    dq,
    dg,
    otc,
    otr,
    obs,
    obr,
    ofin,
    cs,
    cr,
    sb,
    xr,
    fin,
    fout,
    inv,
    wsem,
    qsem,
    ksem,
    kpsem,
    qpsem,
    vsem,
    msem,
    dsem,
    asem,
    osem,
    bsem,
    hsem,
    psem,
    xsem,
    gsem,
):
    me = lax.axis_index("seq")
    mb = lax.axis_index("batch")
    rows, kd = k_ref.shape
    hidden = slope.shape[1]
    heads = wt_ref.shape[0]
    head = kd // heads
    chips = n // 2
    chip = me // 2
    core = me % 2
    pair = chip * 2 + (1 - core)
    cy = chip // SIDE
    cz = chip % SIDE
    load = pltpu.make_async_copy(w_ref, win, wsem)
    load.start()

    def seq_peer(d):
        return lax.rem(me + d, n)

    def chip_peer(d):
        return lax.rem(chip + d, chips)

    def chip_source(d):
        return lax.rem(chip - d + chips, chips)

    def batch_peer(d):
        return lax.rem(mb + d, nb)

    def at(i, size):
        return pl.ds(pl.multiple_of(i * size, size), size)

    barrier = pltpu.get_barrier_semaphore()
    for d in range(1, n):
        pl.semaphore_signal(barrier, inc=1, device_id={"seq": seq_peer(d)}, device_id_type=MESH)
    for d in range(1, nb):
        pl.semaphore_signal(
            barrier, inc=1, device_id={"batch": batch_peer(d)}, device_id_type=MESH
        )

    def turn_values(j, carry):
        vt[at(j, head), :] = v_ref[:, at(j, head)].T
        return carry

    lax.fori_loop(0, kd // head, turn_values, 0)
    pl.semaphore_wait(barrier, n + nb - 2)

    for d in range(1, chips):
        to = chip_peer(d)
        copy = copy_to(
            k_ref.at[:, at(to // 2, head)], kg.at[me], ksem, (), {"seq": to * 2 + core}
        )
        copy.start()
    copy_to(k_ref.at[:, at(chip // 2, head)], kg.at[me], kpsem, (), {"seq": pair}).start()
    for d in range(1, n):
        to = seq_peer(d)
        copy = copy_to(
            q_ref.at[:, at(to, head)], qg.at[me], qsem, (), {"seq": to}
        )
        copy.start()
    vpart = kd // chips
    value_base = 2 * head + vpart
    qg[me] = q_ref[:, at(me, head)]
    qo[at(chip, rows), :] = q_ref[:, at(pair, head)]
    kg[me] = k_ref[:, at(chip // 2, head)]
    ft[pl.ds(value_base, vpart), at(chip, rows)] = vt[at(chip, vpart), :]

    def invert(p, carry):
        found = jnp.int32(0)
        for s in range(n):
            found = jnp.where(order_ref[0, s] == p, jnp.int32(s), found)
        inv[p] = found
        return carry

    lax.fori_loop(0, n, invert, 0)
    load.wait()
    tile = hidden // 4

    def project(j, carry):
        span = at(j, tile)
        value = b_ref[:, span]
        base = 0
        for ref in (q_ref, k_ref, v_ref):
            depth = ref.shape[1]
            value = value + jnp.dot(
                ref[...], win[base : base + depth, span], preferred_element_type=F32
            )
            base += depth
        sig = jax.nn.sigmoid(value)
        slope[:, span] = sig * (1.0 + value * (1.0 - sig))
        act[:, span] = (value * sig).astype(BF16)
        return carry

    lax.fori_loop(0, 4, project, 0)
    lanes = hidden // CLASSES
    for k in range(CLASSES):
        fixed = jnp.floor((slope[:, k * lanes : (k + 1) * lanes] - 0.5) * FIXED + 0.5)
        dq[k, at(chip, rows), :] = fixed.astype(jnp.int32).astype(jnp.int16)

    LAST = SIDE + 3

    def place(k, a, b):
        dy, dz = (a, b) if k < 2 else (b, a)
        return lax.rem(cy + SIDE - dy, SIDE) * SIDE + lax.rem(cz + SIDE - dz, SIDE)

    def toward(k):
        return (1, 1, 3) if k % 2 == 0 else (-1, 3, 1)

    def slot(k, a, b):
        move, near, far = toward(k)
        if b == 0:
            return a - 1
        return 3 + a if b == near else LAST

    def forward(k, a, b, axis, move):
        along_y = (axis == 0) == (k < 2)
        if along_y:
            to = lax.rem(cy + SIDE + move, SIDE) * SIDE + cz
        else:
            to = cy * SIDE + lax.rem(cz + SIDE + move, SIDE)
        a2, b2 = ((a + move) % SIDE, b) if axis == 0 else (a, (b + move) % SIDE)
        part = dq.at[k, at(place(k, a, b), rows)]
        pltpu.make_async_remote_copy(
            src_ref=part,
            dst_ref=part,
            send_sem=asem.at[CLASSES, 0],
            recv_sem=asem.at[k, slot(k, a2, b2)],
            device_id={"seq": to * 2 + core},
            device_id_type=MESH,
        ).start()

    def gathered(ref, k, i):
        return pltpu.make_async_remote_copy(
            src_ref=ref,
            dst_ref=ref,
            send_sem=asem.at[CLASSES, 0],
            recv_sem=asem.at[k, i],
            device_id={"seq": me},
            device_id_type=MESH,
        )

    def arrive(k, a, b):
        gathered(dq.at[k, at(place(k, a, b), rows)], k, slot(k, a, b)).wait_recv()

    def stage0():
        for axis in (0, 1):
            for k in range(CLASSES):
                for move in (1, -1):
                    forward(k, 0, 0, axis, move)

    def stage1():
        for k in range(CLASSES):
            move, near, far = toward(k)
            arrive(k, near, 0)
            forward(k, near, 0, 0, move)
            forward(k, near, 0, 1, 1)
            forward(k, near, 0, 1, -1)
        for k in range(CLASSES):
            move, near, far = toward(k)
            arrive(k, far, 0)
            forward(k, far, 0, 1, 1)
            forward(k, far, 0, 1, -1)

    def stage2():
        for k in range(CLASSES):
            move, near, far = toward(k)
            arrive(k, 0, near)
            forward(k, 0, near, 1, move)
        for k in range(CLASSES):
            arrive(k, 2, 0)
            forward(k, 2, 0, 1, 1)
            forward(k, 2, 0, 1, -1)

    def stage3():
        for a in (0, 1):
            for k in range(CLASSES):
                move, near, far = toward(k)
                line = near if a == 0 else far
                arrive(k, line, near)
                forward(k, line, near, 1, move)

    def stage4():
        for k in range(CLASSES):
            move, near, far = toward(k)
            arrive(k, 2, near)
            forward(k, 2, near, 1, move)

    def stage5():
        for k in range(CLASSES):
            gathered(dq.at[k, pl.ds(0, 2 * SIDE * rows)], k, LAST).wait_recv()

    stage0()
    wt32 = wt_ref[...].astype(F32)
    wt = jnp.concatenate([wt32, jnp.zeros_like(wt32)], axis=0).astype(BF16)
    group_index = lax.broadcasted_iota(jnp.int32, (heads, 1), 0)
    bias = jnp.zeros((heads, 1), F32)
    for g in range(heads):
        bias = jnp.where(group_index == g, bias_ref[0, g], bias)
    predg[chip] = (
        lax.dot_general(wt, act[...], (((1,), (1,)), ((), ())), preferred_element_type=F32)[:heads]
        + bias
    )
    for d in range(1, chips):
        copy = copy_to(
            predg.at[chip], predg.at[chip], dsem, (), {"seq": chip_peer(d) * 2 + core}
        )
        copy.start()

    waits = {
        "key_far": waiter(kg.at[pl.ds(0, chips - 1)], ksem, ()),
        "key_near": waiter(kg.at[pl.ds(0, chips)], kpsem, ()),
        "query": waiter(qg.at[pl.ds(0, n - 1)], qsem, ()),
        "query_near": waiter(qo.at[pl.ds(0, (chips - 1) * rows)], qpsem, ()),
        "value": waiter(
            ft.at[pl.ds(value_base, vpart), pl.ds(0, (chips - 1) * rows)], vsem, ()
        ),
        "mass": waiter(mr.at[pl.ds(0, n - 1)], msem, ()),
        "pred": waiter(predg.at[pl.ds(0, chips - 1)], dsem, ()),
    }
    waits["key_far"].wait_recv()
    for d in range(1, chips):
        held = kg.at[chip_source(d) * 2 + core]
        copy_to(held, held, kpsem, (), {"seq": pair}).start()
    waits["query"].wait_recv()
    for d in range(1, chips):
        source = chip_source(d)
        copy_to(
            qg.at[source * 2 + (1 - core)],
            qo.at[at(source, rows)],
            qpsem,
            (),
            {"seq": pair},
        ).start()
    waits["key_near"].wait_recv()

    limit = limit_ref[0]

    def sort_keys(p, carry):
        ks[at(p, rows), :] = kg[inv[p]]
        return carry

    lax.fori_loop(0, n, sort_keys, 0, unroll=8)
    colacc[...] = jnp.zeros_like(colacc)
    step = 4
    wide = step * rows
    tall = 2 * rows
    row_index = lax.broadcasted_iota(jnp.int32, (tall, 1), 0)
    lane_wide = lax.broadcasted_iota(jnp.int32, (1, wide), 1)

    for w in range(n // step):

        def query_block(t, carry, w=w):
            block = w * step + 2 * t
            queries = jnp.concatenate([qg[inv[block]], qg[inv[block + 1]]], axis=0)
            best = None
            for kc in range(w + 1):
                score = lax.dot_general(
                    queries,
                    ks[kc * wide : (kc + 1) * wide, :],
                    (((1,), (1,)), ((), ())),
                    preferred_element_type=F32,
                )
                if kc == w:
                    score = jnp.where(lane_wide <= row_index + t * tall, score, -1e30)
                sref[:, kc * wide : (kc + 1) * wide] = score
                for j in range(step):
                    part = score[:, j * rows : (j + 1) * rows]
                    best = part if best is None else jnp.maximum(best, part)
            top = jnp.max(best, axis=1, keepdims=True)
            total = None
            for kb in range((w + 1) * step):
                span = slice(kb * rows, (kb + 1) * rows)
                weight = jnp.exp2((sref[:, span] - top) * (scale * LOG2E))
                sref[:, span] = weight
                total = weight if total is None else total + weight
            denom = jnp.sum(total, axis=1, keepdims=True)
            live = (row_index + block * rows < limit).astype(F32)
            share = live / denom
            for kb in range((w + 1) * step):
                span = slice(kb * rows, (kb + 1) * rows)
                part = sref[:, span] * share
                colacc[kb] += jnp.sum(part.reshape(tall // 8, 8, rows), axis=0)
            return carry

        if w == n // step - 1:
            lax.fori_loop(0, 1, query_block, 0)
            stage3()
            lax.fori_loop(1, 2, query_block, 0)
        else:
            lax.fori_loop(0, 2, query_block, 0)
        if w == 3:
            stage1()
        elif w == 5:
            stage2()

    for t in range(n):
        mp[t % 2, t // 2 : t // 2 + 1, :] = jnp.sum(
            colacc[order_ref[0, t]], axis=0, keepdims=True
        )
    for d in range(1, n):
        to = seq_peer(d)
        copy_to(mp.at[to % 2], mr.at[me], msem, (), {"seq": to}).start()
    mr[me] = mp[core]

    waits["query_near"].wait_recv()

    def turn_features(s, carry):
        ft[at(core, head), at(s, rows)] = qg[2 * s + core].T
        ft[at(1 - core, head), at(s, rows)] = qo[at(s, rows), :].T
        kt[:, at(s, rows)] = kg[2 * s + core].T
        return carry

    lax.fori_loop(0, chips, turn_features, 0, unroll=4)
    ft[pl.ds(2 * head, vpart), :] = kt[at(chip % 2, vpart), :]
    stage4()
    for d in range(1, chips):
        to = chip_peer(d)
        copy = copy_to(
            vt.at[at(to, vpart)],
            ft.at[pl.ds(value_base, vpart), at(chip, rows)],
            vsem,
            (),
            {"seq": to * 2 + core},
        )
        copy.start()

    waits["pred"].wait_recv()
    waits["mass"].wait_recv()
    per_group = n // heads
    labels = []
    for g in range(heads):
        value = mr[g * per_group]
        for j in range(1, per_group):
            value = value + mr[g * per_group + j]
        labels.append(jnp.log1p(value))
    lane = lax.broadcasted_iota(jnp.int32, (1, rows), 1)
    for s in range(chips):
        label = jnp.concatenate([part[s : s + 1] for part in labels], axis=0)
        live_row = (lane + order_ref[0, 2 * s + core] * rows < limit).astype(F32)
        resid = ((predg[s] - label) * live_row * norm).astype(BF16).astype(F32)
        resid = jnp.concatenate([resid, jnp.zeros_like(resid)], axis=0)
        rs[s] = resid
        rt[s * rows : (s + 1) * rows, :] = resid.T.astype(BF16)

    per_round = CLASSES // ROUNDS

    def delta_round(r):
        base = r * per_round

        many = 4 * rows

        def tokens(s, carry):
            back = jnp.dot(
                rt[at(s, many), :],
                wt[:, base * lanes : (base + per_round) * lanes],
                preferred_element_type=F32,
            )
            for j in range(per_round):
                held = dq[base + j, at(s, many), :].astype(jnp.int32).astype(F32)
                value = back[:, j * lanes : (j + 1) * lanes] * (held * (1.0 / FIXED) + 0.5)
                dg[base + j, at(s, many), :] = value.astype(BF16)
            return carry

        lax.fori_loop(0, chips // 4, tokens, 0)

    half = ft.shape[0] // 2
    piece = hidden // ROUNDS
    share_rows = half // GRAN // nb

    def term(r, which):
        lhs = ft[at(which, half), :]
        parts = [
            jnp.dot(lhs, dg[r * per_round + j], preferred_element_type=F32)
            for j in range(per_round)
        ]
        return jnp.concatenate(parts, axis=1)

    def start_of(target):
        return lax.rem(share_rows * target + 2 * SIDE * chip, half // GRAN)

    swaps = []

    def swap(r):
        cs[r] = term(r, 1 - core)
        copy = copy_to(cs.at[r], cr.at[r], psem, (r,), {"seq": pair})
        copy.start()
        swaps.append(copy)

    def reduce_chip(r):
        own = term(r, core)
        swaps[r].wait_recv()
        both = (own + cr[r]).reshape(half // GRAN, GRAN, piece)
        sb[r, : half // GRAN] = both
        sb[r, half // GRAN :] = both[: share_rows - 1]
        for d in (2, 1, 3):
            to = batch_peer(d)
            copy = copy_to(
                sb.at[r, pl.ds(start_of(to), share_rows)],
                xr.at[r, d - 1],
                xsem,
                (r,),
                {"batch": to},
            )
            copy.start()

    def granule(i):
        q_gran = 2 * head // GRAN
        k_gran = vpart // GRAN
        total_q = n * head // GRAN
        total_k = kd // GRAN
        return jnp.where(
            i < q_gran,
            q_gran * chip + i,
            jnp.where(
                i < q_gran + k_gran,
                total_q + k_gran * chip + i - q_gran,
                total_q + total_k + k_gran * chip + i - q_gran - k_gran,
            ),
        )

    per_dev = share_rows * nb

    def owner_of(e):
        o = lax.rem(start_of(mb) + e, half // GRAN)
        return granule(o + core * (half // GRAN)) // per_dev

    def maker_of(e):
        q_gran = 2 * head // GRAN
        k_gran = vpart // GRAN
        total_q = n * head // GRAN
        total_k = kd // GRAN
        u = per_dev * me + share_rows * mb + e
        uk = u - total_q
        uv = uk - total_k
        which = jnp.where(
            uk < 0, u // q_gran, jnp.where(uv < 0, uk // k_gran, uv // k_gran)
        )
        i = jnp.where(
            uk < 0,
            u % q_gran,
            jnp.where(uv < 0, q_gran + uk % k_gran, q_gran + k_gran + uv % k_gran),
        )
        return which * 2 + jnp.where(i >= half // GRAN, 1, 0)

    def final_copy(r, e):
        return copy_to(fin.at[r, e], fout.at[r, e], gsem, (e,), {"seq": owner_of(e)})

    def finish(r):
        value = sb[r, pl.ds(start_of(mb), share_rows)]
        waiter(xr.at[r], xsem, (r,)).wait_recv()
        for d in range(nb - 1):
            value = value + xr[r, d]
        fin[r] = value
        for e in range(share_rows):
            stays = owner_of(e) == me

            @pl.when(jnp.logical_not(stays))
            def _(r=r, e=e):
                final_copy(r, e).start()

            @pl.when(stays)
            def _(r=r, e=e):
                fout[r, e] = fin[r, e]

    every = n // otc.shape[0]
    pieces = otc.shape[0]
    reduces = lax.rem(me, every) == 0
    resid32 = rs[chip]
    out_term = jnp.dot(resid32.astype(BF16), act[...], preferred_element_type=F32)[:heads]
    lane_row = lax.broadcasted_iota(jnp.int32, (heads, rows), 1)
    bias_row = jnp.sum(
        jnp.where(
            lane_row == group_index, jnp.sum(resid32[:heads], axis=1, keepdims=True), 0.0
        ),
        axis=0,
        keepdims=True,
    )
    delta = (
        jnp.dot(resid32.T.astype(BF16), wt, preferred_element_type=F32) * slope[...]
    ).astype(BF16)
    delta_sum = jnp.sum(delta.astype(F32), axis=0, keepdims=True)
    filler = jnp.zeros((heads - 2, rows), F32)
    for p in range(pieces):
        span = slice(p * rows, (p + 1) * rows)
        otc[p] = jnp.concatenate([out_term[:, span], delta_sum[:, span], bias_row, filler], axis=0)

    def small_copy(p):
        return copy_to(otc.at[p], otr.at[me], osem, (), {"seq": jnp.int32(p * every)})

    for p in range(pieces):

        @pl.when(me != p * every)
        def _(p=p):
            small_copy(p).start()

    stage5()
    delta_round(0)
    waits["value"].wait_recv()
    swap(0)

    def small_over_seq():
        @pl.when(reduces)
        def _():
            otr[me] = otc[me // every]
            waiter(otr.at[pl.ds(0, n - 1)], osem, ()).wait_recv()
            total = otr[0]
            for d in range(1, n):
                total = total + otr[d]
            obs[...] = total
            for d in range(1, nb):
                copy_to(obs, obr.at[d - 1], bsem, (), {"batch": batch_peer(d)}).start()

    def small_over_batch():
        @pl.when(reduces)
        def _():
            waiter(obr, bsem, ()).wait_recv()
            total = obs[...]
            for d in range(nb - 1):
                total = total + obr[d]
            ofin[me // every] = total
            done = ofin.at[me // every]
            for d in range(1, n):
                copy_to(done, done, hsem, (), {"seq": seq_peer(d)}).start()

    for r in range(1, ROUNDS):
        delta_round(r)
        swap(r)
        reduce_chip(r - 1)
        if r == ROUNDS // 2:
            small_over_seq()
    reduce_chip(ROUNDS - 1)
    for r in range(ROUNDS):
        finish(r)
        if r == 1:
            small_over_batch()

    @pl.when(reduces)
    def _():
        waiter(ofin.at[pl.ds(0, pieces - 1)], hsem, ()).wait_recv()

    @pl.when(jnp.logical_not(reduces))
    def _():
        waiter(ofin, hsem, ()).wait_recv()

    small = jnp.concatenate([ofin[p] for p in range(pieces)], axis=1)
    small_ref[...] = small
    for e in range(share_rows):

        @pl.when(maker_of(e) != me)
        def _(e=e):
            waiter(fout.at[:, e], gsem, (e,)).wait_recv()

        for r in range(ROUNDS):
            grad_ref[e * GRAN : (e + 1) * GRAN, r * piece : (r + 1) * piece] = fout[r, e]
    for wait in waits.values():
        wait.wait_send()
    gathered(dq.at[:, pl.ds(0, (SIDE * SIDE - 1) * rows)], 0, 0).wait_send()

    @pl.when(reduces)
    def _():
        waiter(otc.at[pl.ds(0, pieces - 1)], osem, ()).wait_send()
        waiter(obr, bsem, ()).wait_send()
        waiter(otr.at[pl.ds(0, n - 1)], hsem, ()).wait_send()

    @pl.when(jnp.logical_not(reduces))
    def _():
        waiter(otc, osem, ()).wait_send()

    for r in range(ROUNDS):
        swaps[r].wait_send()
        waiter(xr.at[r], xsem, (r,)).wait_send()
    for e in range(share_rows):

        @pl.when(owner_of(e) != me)
        def _(e=e):
            waiter(fin.at[:, e], gsem, (e,)).wait_send()


def emit(grad_in, small_in, grad_ref, gw_ref, gb_ref, ob_ref):
    heads = gw_ref.shape[0]
    grad_ref[...] = grad_in[...]
    gw_ref[...] = small_in[:heads]
    gb_ref[...] = small_in[heads : heads + 1]
    ob_ref[...] = small_in[heads + 1 : heads + 2, :heads]


def on_device(queries, keys, values, lengths, block_pos, w_in, b_in, output_weight, output_bias):
    n = lax.axis_size("seq")
    nb = lax.axis_size("batch")
    q_rows = queries[0]
    k_rows = keys[0]
    v_rows = values[0]
    rows, kd = k_rows.shape
    heads = output_weight.shape[1]
    hidden = w_in.shape[1]
    feat = w_in.shape[0]
    head = kd // heads
    scale = 1.0 / math.sqrt(head)
    norm = 1.0 / math.sqrt(nb * n * rows)
    vmem = pl.BlockSpec(memory_space=pltpu.VMEM)
    total = n * rows
    chips = n // 2
    part = feat // n // nb
    chip_feat = feat // chips
    piece = hidden // ROUNDS
    grans = chip_feat // 2 // GRAN
    share_rows = grans // nb
    dma = pltpu.SemaphoreType.DMA
    grad, small = pl.pallas_call(
        functools.partial(kernel, n, nb, norm, scale),
        out_shape=(
            jax.ShapeDtypeStruct((part, hidden), F32),
            jax.ShapeDtypeStruct((2 * heads, hidden), F32),
        ),
        in_specs=[vmem] * 3
        + [pl.BlockSpec(memory_space=pl.ANY)]
        + [vmem] * 2
        + [pl.BlockSpec(memory_space=pltpu.SMEM)] * 3,
        out_specs=(vmem, vmem),
        scratch_shapes=[
            pltpu.VMEM((feat, hidden), BF16),
            pltpu.VMEM((n, rows, head), BF16),
            pltpu.VMEM((n, rows, head), BF16),
            pltpu.VMEM((total, head), BF16),
            pltpu.VMEM((total // 2, head), BF16),
            pltpu.VMEM((head, total // 2), BF16),
            pltpu.VMEM((chip_feat, total // 2), BF16),
            pltpu.VMEM((kd, rows), BF16),
            pltpu.VMEM((rows, hidden), F32),
            pltpu.VMEM((rows, hidden), BF16),
            pltpu.VMEM((2 * rows, total), F32),
            pltpu.VMEM((n, 8, rows), F32),
            pltpu.VMEM((2, chips, rows), F32),
            pltpu.VMEM((n, chips, rows), F32),
            pltpu.VMEM((chips, heads, rows), F32),
            pltpu.VMEM((chips, 2 * heads, rows), F32),
            pltpu.VMEM((total // 2, 2 * heads), BF16),
            pltpu.VMEM((CLASSES, total // 2, hidden // CLASSES), jnp.int16),
            pltpu.VMEM((CLASSES, total // 2, hidden // CLASSES), BF16),
            pltpu.VMEM((hidden // rows, 2 * heads, rows), F32),
            pltpu.VMEM((n, 2 * heads, rows), F32),
            pltpu.VMEM((2 * heads, rows), F32),
            pltpu.VMEM((nb - 1, 2 * heads, rows), F32),
            pltpu.VMEM((hidden // rows, 2 * heads, rows), F32),
            pltpu.VMEM((ROUNDS, chip_feat // 2, piece), F32),
            pltpu.VMEM((ROUNDS, chip_feat // 2, piece), F32),
            pltpu.VMEM((ROUNDS, grans + share_rows - 1, GRAN, piece), F32),
            pltpu.VMEM((ROUNDS, nb - 1, share_rows, GRAN, piece), F32),
            pltpu.VMEM((ROUNDS, share_rows, GRAN, piece), F32),
            pltpu.VMEM((ROUNDS, share_rows, GRAN, piece), F32),
            pltpu.SMEM((n,), jnp.int32),
            dma,
            dma((2,)),
            dma((2,)),
            dma((2,)),
            dma((2,)),
            dma((2,)),
            dma((2,)),
            dma((2,)),
            dma((CLASSES + 1, SIDE + 4)),
            dma((2,)),
            dma((2,)),
            dma((2,)),
            dma((2, ROUNDS)),
            dma((2, ROUNDS)),
            dma((2, share_rows)),
        ],
        compiler_params=pltpu.CompilerParams(
            collective_id=0, has_side_effects=True, vmem_limit_bytes=60 * 1024 * 1024
        ),
    )(
        q_rows,
        k_rows,
        v_rows,
        w_in,
        b_in[None, :],
        output_weight.T,
        output_bias[None, :],
        block_pos,
        lengths,
    )
    grad, gw, gb, ob = pl.pallas_call(
        emit,
        out_shape=(
            jax.ShapeDtypeStruct((part, hidden), F32),
            jax.ShapeDtypeStruct((heads, hidden), F32),
            jax.ShapeDtypeStruct((1, hidden), F32),
            jax.ShapeDtypeStruct((1, heads), F32),
        ),
        in_specs=[vmem] * 2,
        out_specs=(vmem,) * 4,
    )(grad, small)
    return (grad, gb[0], gw.T, ob[0])


def solution(mesh):
    return jax.shard_map(
        on_device,
        mesh=mesh,
        in_specs=(
            P("batch", "seq", None),
            P("batch", "seq", None),
            P("batch", "seq", None),
            P("batch"),
            P("batch", None),
            P(),
            P(),
            P(),
            P(),
        ),
        out_specs=(P(("seq", "batch"), None), P(), P(), P()),
        check_vma=False,
    )
```

```python
import functools
import math

import jax
import jax.numpy as jnp
from jax import lax
from jax.experimental import pallas as pl
from jax.experimental.pallas import tpu as pltpu
from jax.sharding import PartitionSpec as P

F32 = jnp.float32
BF16 = jnp.bfloat16
MESH = pl.DeviceIdType.MESH
SIDE = 4
ROUNDS = 4
CLASSES = 4
FIXED = 54000.0
GRAN = 16
LOG2E = 1.4426950408889634


def waiter(ref, sems, index):
    return pltpu.make_async_remote_copy(
        src_ref=ref,
        dst_ref=ref,
        send_sem=sems.at[(0, *index)],
        recv_sem=sems.at[(1, *index)],
        device_id={"seq": lax.axis_index("seq")},
        device_id_type=MESH,
    )


def copy_to(src, dst, sems, index, target):
    return pltpu.make_async_remote_copy(
        src_ref=src,
        dst_ref=dst,
        send_sem=sems.at[(0, *index)],
        recv_sem=sems.at[(1, *index)],
        device_id=target,
        device_id_type=MESH,
    )


def kernel(
    n,
    nb,
    norm,
    scale,
    q_ref,
    k_ref,
    v_ref,
    w_ref,
    b_ref,
    wt_ref,
    bias_ref,
    order_ref,
    limit_ref,
    grad_ref,
    small_ref,
    win,
    qg,
    kg,
    ks,
    qo,
    kt,
    ft,
    vt,
    slope,
    act,
    sref,
    colacc,
    mp,
    mr,
    predg,
    rs,
    rt,
    dq,
    dg,
    otc,
    otr,
    obs,
    obr,
    ofin,
    cs,
    cr,
    sb,
    xr,
    fin,
    fout,
    inv,
    wsem,
    qsem,
    ksem,
    kpsem,
    qpsem,
    vsem,
    msem,
    dsem,
    asem,
    osem,
    bsem,
    hsem,
    psem,
    xsem,
    gsem,
):
    me = lax.axis_index("seq")
    mb = lax.axis_index("batch")
    rows, kd = k_ref.shape
    hidden = slope.shape[1]
    heads = wt_ref.shape[0]
    head = kd // heads
    chips = n // 2
    chip = me // 2
    core = me % 2
    pair = chip * 2 + (1 - core)
    cy = chip // SIDE
    cz = chip % SIDE
    load = pltpu.make_async_copy(w_ref, win, wsem)
    load.start()

    def seq_peer(d):
        return lax.rem(me + d, n)

    def chip_peer(d):
        return lax.rem(chip + d, chips)

    def chip_source(d):
        return lax.rem(chip - d + chips, chips)

    def batch_peer(d):
        return lax.rem(mb + d, nb)

    def at(i, size):
        return pl.ds(pl.multiple_of(i * size, size), size)

    barrier = pltpu.get_barrier_semaphore()
    for d in range(1, n):
        pl.semaphore_signal(barrier, inc=1, device_id={"seq": seq_peer(d)}, device_id_type=MESH)
    for d in range(1, nb):
        pl.semaphore_signal(
            barrier, inc=1, device_id={"batch": batch_peer(d)}, device_id_type=MESH
        )

    def turn_values(j, carry):
        vt[at(j, head), :] = v_ref[:, at(j, head)].T
        return carry

    lax.fori_loop(0, kd // head, turn_values, 0)
    pl.semaphore_wait(barrier, n + nb - 2)

    for d in range(1, chips):
        to = chip_peer(d)
        copy = copy_to(
            k_ref.at[:, at(to // 2, head)], kg.at[me], ksem, (), {"seq": to * 2 + core}
        )
        copy.start()
    copy_to(k_ref.at[:, at(chip // 2, head)], kg.at[me], kpsem, (), {"seq": pair}).start()
    for d in range(1, n):
        to = seq_peer(d)
        copy = copy_to(
            q_ref.at[:, at(to, head)], qg.at[me], qsem, (), {"seq": to}
        )
        copy.start()
    vpart = kd // chips
    value_base = 2 * head + vpart
    qg[me] = q_ref[:, at(me, head)]
    qo[at(chip, rows), :] = q_ref[:, at(pair, head)]
    kg[me] = k_ref[:, at(chip // 2, head)]
    ft[pl.ds(value_base, vpart), at(chip, rows)] = vt[at(chip, vpart), :]

    def invert(p, carry):
        found = jnp.int32(0)
        for s in range(n):
            found = jnp.where(order_ref[0, s] == p, jnp.int32(s), found)
        inv[p] = found
        return carry

    lax.fori_loop(0, n, invert, 0)
    load.wait()
    tile = hidden // 4

    def project(j, carry):
        span = at(j, tile)
        value = b_ref[:, span]
        base = 0
        for ref in (q_ref, k_ref, v_ref):
            depth = ref.shape[1]
            value = value + jnp.dot(
                ref[...], win[base : base + depth, span], preferred_element_type=F32
            )
            base += depth
        sig = jax.nn.sigmoid(value)
        slope[:, span] = sig * (1.0 + value * (1.0 - sig))
        act[:, span] = (value * sig).astype(BF16)
        return carry

    lax.fori_loop(0, 4, project, 0)
    lanes = hidden // CLASSES
    for k in range(CLASSES):
        fixed = jnp.floor((slope[:, k * lanes : (k + 1) * lanes] - 0.5) * FIXED + 0.5)
        dq[k, at(chip, rows), :] = fixed.astype(jnp.int32).astype(jnp.int16)

    LAST = SIDE + 3

    def place(k, a, b):
        dy, dz = (a, b) if k < 2 else (b, a)
        return lax.rem(cy + SIDE - dy, SIDE) * SIDE + lax.rem(cz + SIDE - dz, SIDE)

    def toward(k):
        return (1, 1, 3) if k % 2 == 0 else (-1, 3, 1)

    def slot(k, a, b):
        move, near, far = toward(k)
        if b == 0:
            return a - 1
        return 3 + a if b == near else LAST

    def forward(k, a, b, axis, move):
        along_y = (axis == 0) == (k < 2)
        if along_y:
            to = lax.rem(cy + SIDE + move, SIDE) * SIDE + cz
        else:
            to = cy * SIDE + lax.rem(cz + SIDE + move, SIDE)
        a2, b2 = ((a + move) % SIDE, b) if axis == 0 else (a, (b + move) % SIDE)
        part = dq.at[k, at(place(k, a, b), rows)]
        pltpu.make_async_remote_copy(
            src_ref=part,
            dst_ref=part,
            send_sem=asem.at[CLASSES, 0],
            recv_sem=asem.at[k, slot(k, a2, b2)],
            device_id={"seq": to * 2 + core},
            device_id_type=MESH,
        ).start()

    def gathered(ref, k, i):
        return pltpu.make_async_remote_copy(
            src_ref=ref,
            dst_ref=ref,
            send_sem=asem.at[CLASSES, 0],
            recv_sem=asem.at[k, i],
            device_id={"seq": me},
            device_id_type=MESH,
        )

    def arrive(k, a, b):
        gathered(dq.at[k, at(place(k, a, b), rows)], k, slot(k, a, b)).wait_recv()

    def stage0():
        for axis in (0, 1):
            for k in range(CLASSES):
                for move in (1, -1):
                    forward(k, 0, 0, axis, move)

    def stage1():
        for k in range(CLASSES):
            move, near, far = toward(k)
            arrive(k, near, 0)
            forward(k, near, 0, 0, move)
            forward(k, near, 0, 1, 1)
            forward(k, near, 0, 1, -1)
        for k in range(CLASSES):
            move, near, far = toward(k)
            arrive(k, far, 0)
            forward(k, far, 0, 1, 1)
            forward(k, far, 0, 1, -1)

    def stage2():
        for k in range(CLASSES):
            move, near, far = toward(k)
            arrive(k, 0, near)
            forward(k, 0, near, 1, move)
        for k in range(CLASSES):
            arrive(k, 2, 0)
            forward(k, 2, 0, 1, 1)
            forward(k, 2, 0, 1, -1)

    def stage3():
        for a in (0, 1):
            for k in range(CLASSES):
                move, near, far = toward(k)
                line = near if a == 0 else far
                arrive(k, line, near)
                forward(k, line, near, 1, move)

    def stage4():
        for k in range(CLASSES):
            move, near, far = toward(k)
            arrive(k, 2, near)
            forward(k, 2, near, 1, move)

    def stage5():
        for k in range(CLASSES):
            gathered(dq.at[k, pl.ds(0, 2 * SIDE * rows)], k, LAST).wait_recv()

    stage0()
    wt32 = wt_ref[...].astype(F32)
    wt = jnp.concatenate([wt32, jnp.zeros_like(wt32)], axis=0).astype(BF16)
    group_index = lax.broadcasted_iota(jnp.int32, (heads, 1), 0)
    bias = jnp.zeros((heads, 1), F32)
    for g in range(heads):
        bias = jnp.where(group_index == g, bias_ref[0, g], bias)
    predg[chip] = (
        lax.dot_general(wt, act[...], (((1,), (1,)), ((), ())), preferred_element_type=F32)[:heads]
        + bias
    )
    for d in range(1, chips):
        copy = copy_to(
            predg.at[chip], predg.at[chip], dsem, (), {"seq": chip_peer(d) * 2 + core}
        )
        copy.start()

    waits = {
        "key_far": waiter(kg.at[pl.ds(0, chips - 1)], ksem, ()),
        "key_near": waiter(kg.at[pl.ds(0, chips)], kpsem, ()),
        "query": waiter(qg.at[pl.ds(0, n - 1)], qsem, ()),
        "query_near": waiter(qo.at[pl.ds(0, (chips - 1) * rows)], qpsem, ()),
        "value": waiter(
            ft.at[pl.ds(value_base, vpart), pl.ds(0, (chips - 1) * rows)], vsem, ()
        ),
        "mass": waiter(mr.at[pl.ds(0, n - 1)], msem, ()),
        "pred": waiter(predg.at[pl.ds(0, chips - 1)], dsem, ()),
    }
    waits["key_far"].wait_recv()
    for d in range(1, chips):
        held = kg.at[chip_source(d) * 2 + core]
        copy_to(held, held, kpsem, (), {"seq": pair}).start()
    waits["query"].wait_recv()
    for d in range(1, chips):
        source = chip_source(d)
        copy_to(
            qg.at[source * 2 + (1 - core)],
            qo.at[at(source, rows)],
            qpsem,
            (),
            {"seq": pair},
        ).start()
    waits["key_near"].wait_recv()

    limit = limit_ref[0]

    def sort_keys(p, carry):
        ks[at(p, rows), :] = kg[inv[p]]
        return carry

    lax.fori_loop(0, n, sort_keys, 0, unroll=8)
    colacc[...] = jnp.zeros_like(colacc)
    step = 4
    wide = step * rows
    tall = 2 * rows
    row_index = lax.broadcasted_iota(jnp.int32, (tall, 1), 0)
    lane_wide = lax.broadcasted_iota(jnp.int32, (1, wide), 1)

    for w in range(n // step):

        def query_block(t, carry, w=w):
            block = w * step + 2 * t
            queries = jnp.concatenate([qg[inv[block]], qg[inv[block + 1]]], axis=0)
            best = None
            for kc in range(w + 1):
                score = lax.dot_general(
                    queries,
                    ks[kc * wide : (kc + 1) * wide, :],
                    (((1,), (1,)), ((), ())),
                    preferred_element_type=F32,
                )
                if kc == w:
                    score = jnp.where(lane_wide <= row_index + t * tall, score, -1e30)
                sref[:, kc * wide : (kc + 1) * wide] = score
                for j in range(step):
                    part = score[:, j * rows : (j + 1) * rows]
                    best = part if best is None else jnp.maximum(best, part)
            top = jnp.max(best, axis=1, keepdims=True)
            total = None
            for kb in range((w + 1) * step):
                span = slice(kb * rows, (kb + 1) * rows)
                weight = jnp.exp2((sref[:, span] - top) * (scale * LOG2E))
                sref[:, span] = weight
                total = weight if total is None else total + weight
            denom = jnp.sum(total, axis=1, keepdims=True)
            live = (row_index + block * rows < limit).astype(F32)
            share = live / denom
            for kb in range((w + 1) * step):
                span = slice(kb * rows, (kb + 1) * rows)
                part = sref[:, span] * share
                colacc[kb] += jnp.sum(part.reshape(tall // 8, 8, rows), axis=0)
            return carry

        if w == n // step - 1:
            lax.fori_loop(0, 1, query_block, 0)
            stage3()
            lax.fori_loop(1, 2, query_block, 0)
        else:
            lax.fori_loop(0, 2, query_block, 0)
        if w == 3:
            stage1()
        elif w == 5:
            stage2()

    for t in range(n):
        mp[t % 2, t // 2 : t // 2 + 1, :] = jnp.sum(
            colacc[order_ref[0, t]], axis=0, keepdims=True
        )
    for d in range(1, n):
        to = seq_peer(d)
        copy_to(mp.at[to % 2], mr.at[me], msem, (), {"seq": to}).start()
    mr[me] = mp[core]

    waits["query_near"].wait_recv()

    def turn_features(s, carry):
        ft[at(core, head), at(s, rows)] = qg[2 * s + core].T
        ft[at(1 - core, head), at(s, rows)] = qo[at(s, rows), :].T
        kt[:, at(s, rows)] = kg[2 * s + core].T
        return carry

    lax.fori_loop(0, chips, turn_features, 0, unroll=4)
    ft[pl.ds(2 * head, vpart), :] = kt[at(chip % 2, vpart), :]
    stage4()
    for d in range(1, chips):
        to = chip_peer(d)
        copy = copy_to(
            vt.at[at(to, vpart)],
            ft.at[pl.ds(value_base, vpart), at(chip, rows)],
            vsem,
            (),
            {"seq": to * 2 + core},
        )
        copy.start()

    waits["pred"].wait_recv()
    waits["mass"].wait_recv()
    per_group = n // heads
    labels = []
    for g in range(heads):
        value = mr[g * per_group]
        for j in range(1, per_group):
            value = value + mr[g * per_group + j]
        labels.append(jnp.log1p(value))
    lane = lax.broadcasted_iota(jnp.int32, (1, rows), 1)
    for s in range(chips):
        label = jnp.concatenate([part[s : s + 1] for part in labels], axis=0)
        live_row = (lane + order_ref[0, 2 * s + core] * rows < limit).astype(F32)
        resid = ((predg[s] - label) * live_row * norm).astype(BF16).astype(F32)
        resid = jnp.concatenate([resid, jnp.zeros_like(resid)], axis=0)
        rs[s] = resid
        rt[s * rows : (s + 1) * rows, :] = resid.T.astype(BF16)

    per_round = CLASSES // ROUNDS

    def delta_round(r):
        base = r * per_round

        many = 4 * rows

        def tokens(s, carry):
            back = jnp.dot(
                rt[at(s, many), :],
                wt[:, base * lanes : (base + per_round) * lanes],
                preferred_element_type=F32,
            )
            for j in range(per_round):
                held = dq[base + j, at(s, many), :].astype(jnp.int32).astype(F32)
                value = back[:, j * lanes : (j + 1) * lanes] * (held * (1.0 / FIXED) + 0.5)
                dg[base + j, at(s, many), :] = value.astype(BF16)
            return carry

        lax.fori_loop(0, chips // 4, tokens, 0)

    half = ft.shape[0] // 2
    piece = hidden // ROUNDS
    share_rows = half // GRAN // nb

    def term(r, which):
        lhs = ft[at(which, half), :]
        parts = [
            jnp.dot(lhs, dg[r * per_round + j], preferred_element_type=F32)
            for j in range(per_round)
        ]
        return jnp.concatenate(parts, axis=1)

    def start_of(target):
        return lax.rem(share_rows * target + 2 * SIDE * chip, half // GRAN)

    swaps = []

    def swap(r):
        cs[r] = term(r, 1 - core)
        copy = copy_to(cs.at[r], cr.at[r], psem, (r,), {"seq": pair})
        copy.start()
        swaps.append(copy)

    def reduce_chip(r):
        own = term(r, core)
        swaps[r].wait_recv()
        both = (own + cr[r]).reshape(half // GRAN, GRAN, piece)
        sb[r, : half // GRAN] = both
        sb[r, half // GRAN :] = both[: share_rows - 1]
        for d in (2, 1, 3):
            to = batch_peer(d)
            copy = copy_to(
                sb.at[r, pl.ds(start_of(to), share_rows)],
                xr.at[r, d - 1],
                xsem,
                (r,),
                {"batch": to},
            )
            copy.start()

    def granule(i):
        q_gran = 2 * head // GRAN
        k_gran = vpart // GRAN
        total_q = n * head // GRAN
        total_k = kd // GRAN
        return jnp.where(
            i < q_gran,
            q_gran * chip + i,
            jnp.where(
                i < q_gran + k_gran,
                total_q + k_gran * chip + i - q_gran,
                total_q + total_k + k_gran * chip + i - q_gran - k_gran,
            ),
        )

    per_dev = share_rows * nb

    def owner_of(e):
        o = lax.rem(start_of(mb) + e, half // GRAN)
        return granule(o + core * (half // GRAN)) // per_dev

    def maker_of(e):
        q_gran = 2 * head // GRAN
        k_gran = vpart // GRAN
        total_q = n * head // GRAN
        total_k = kd // GRAN
        u = per_dev * me + share_rows * mb + e
        uk = u - total_q
        uv = uk - total_k
        which = jnp.where(
            uk < 0, u // q_gran, jnp.where(uv < 0, uk // k_gran, uv // k_gran)
        )
        i = jnp.where(
            uk < 0,
            u % q_gran,
            jnp.where(uv < 0, q_gran + uk % k_gran, q_gran + k_gran + uv % k_gran),
        )
        return which * 2 + jnp.where(i >= half // GRAN, 1, 0)

    def final_copy(r, e):
        return copy_to(fin.at[r, e], fout.at[r, e], gsem, (e,), {"seq": owner_of(e)})

    def finish(r):
        value = sb[r, pl.ds(start_of(mb), share_rows)]
        waiter(xr.at[r], xsem, (r,)).wait_recv()
        for d in range(nb - 1):
            value = value + xr[r, d]
        fin[r] = value
        for e in range(share_rows):
            stays = owner_of(e) == me

            @pl.when(jnp.logical_not(stays))
            def _(r=r, e=e):
                final_copy(r, e).start()

            @pl.when(stays)
            def _(r=r, e=e):
                fout[r, e] = fin[r, e]

    stage5()
    delta_round(0)
    waits["value"].wait_recv()
    swap(0)
    every = n // otc.shape[0]
    pieces = otc.shape[0]
    reduces = lax.rem(me, every) == 0
    resid32 = rs[chip]
    out_term = jnp.dot(resid32.astype(BF16), act[...], preferred_element_type=F32)[:heads]
    lane_row = lax.broadcasted_iota(jnp.int32, (heads, rows), 1)
    bias_row = jnp.sum(
        jnp.where(
            lane_row == group_index, jnp.sum(resid32[:heads], axis=1, keepdims=True), 0.0
        ),
        axis=0,
        keepdims=True,
    )
    delta = (
        jnp.dot(resid32.T.astype(BF16), wt, preferred_element_type=F32) * slope[...]
    ).astype(BF16)
    delta_sum = jnp.sum(delta.astype(F32), axis=0, keepdims=True)
    filler = jnp.zeros((heads - 2, rows), F32)
    for p in range(pieces):
        span = slice(p * rows, (p + 1) * rows)
        otc[p] = jnp.concatenate([out_term[:, span], delta_sum[:, span], bias_row, filler], axis=0)

    def small_copy(p):
        return copy_to(otc.at[p], otr.at[me], osem, (), {"seq": jnp.int32(p * every)})

    for p in range(pieces):

        @pl.when(me != p * every)
        def _(p=p):
            small_copy(p).start()


    def small_over_seq():
        @pl.when(reduces)
        def _():
            otr[me] = otc[me // every]
            waiter(otr.at[pl.ds(0, n - 1)], osem, ()).wait_recv()
            total = otr[0]
            for d in range(1, n):
                total = total + otr[d]
            obs[...] = total
            for d in range(1, nb):
                copy_to(obs, obr.at[d - 1], bsem, (), {"batch": batch_peer(d)}).start()

    def small_over_batch():
        @pl.when(reduces)
        def _():
            waiter(obr, bsem, ()).wait_recv()
            total = obs[...]
            for d in range(nb - 1):
                total = total + obr[d]
            ofin[me // every] = total
            done = ofin.at[me // every]
            for d in range(1, n):
                copy_to(done, done, hsem, (), {"seq": seq_peer(d)}).start()

    for r in range(1, ROUNDS):
        delta_round(r)
        swap(r)
        reduce_chip(r - 1)
        if r == ROUNDS // 2:
            small_over_seq()
    reduce_chip(ROUNDS - 1)
    for r in range(ROUNDS):
        finish(r)
        if r == 1:
            small_over_batch()

    @pl.when(reduces)
    def _():
        waiter(ofin.at[pl.ds(0, pieces - 1)], hsem, ()).wait_recv()

    @pl.when(jnp.logical_not(reduces))
    def _():
        waiter(ofin, hsem, ()).wait_recv()

    small = jnp.concatenate([ofin[p] for p in range(pieces)], axis=1)
    small_ref[...] = small
    for e in range(share_rows):

        @pl.when(maker_of(e) != me)
        def _(e=e):
            waiter(fout.at[:, e], gsem, (e,)).wait_recv()

        for r in range(ROUNDS):
            grad_ref[e * GRAN : (e + 1) * GRAN, r * piece : (r + 1) * piece] = fout[r, e]
    for wait in waits.values():
        wait.wait_send()
    gathered(dq.at[:, pl.ds(0, (SIDE * SIDE - 1) * rows)], 0, 0).wait_send()

    @pl.when(reduces)
    def _():
        waiter(otc.at[pl.ds(0, pieces - 1)], osem, ()).wait_send()
        waiter(obr, bsem, ()).wait_send()
        waiter(otr.at[pl.ds(0, n - 1)], hsem, ()).wait_send()

    @pl.when(jnp.logical_not(reduces))
    def _():
        waiter(otc, osem, ()).wait_send()

    for r in range(ROUNDS):
        swaps[r].wait_send()
        waiter(xr.at[r], xsem, (r,)).wait_send()
    for e in range(share_rows):

        @pl.when(owner_of(e) != me)
        def _(e=e):
            waiter(fin.at[:, e], gsem, (e,)).wait_send()


def emit(grad_in, small_in, grad_ref, gw_ref, gb_ref, ob_ref):
    heads = gw_ref.shape[0]
    grad_ref[...] = grad_in[...]
    gw_ref[...] = small_in[:heads]
    gb_ref[...] = small_in[heads : heads + 1]
    ob_ref[...] = small_in[heads + 1 : heads + 2, :heads]


def on_device(queries, keys, values, lengths, block_pos, w_in, b_in, output_weight, output_bias):
    n = lax.axis_size("seq")
    nb = lax.axis_size("batch")
    q_rows = queries[0]
    k_rows = keys[0]
    v_rows = values[0]
    rows, kd = k_rows.shape
    heads = output_weight.shape[1]
    hidden = w_in.shape[1]
    feat = w_in.shape[0]
    head = kd // heads
    scale = 1.0 / math.sqrt(head)
    norm = 1.0 / math.sqrt(nb * n * rows)
    vmem = pl.BlockSpec(memory_space=pltpu.VMEM)
    total = n * rows
    chips = n // 2
    part = feat // n // nb
    chip_feat = feat // chips
    piece = hidden // ROUNDS
    grans = chip_feat // 2 // GRAN
    share_rows = grans // nb
    dma = pltpu.SemaphoreType.DMA
    grad, small = pl.pallas_call(
        functools.partial(kernel, n, nb, norm, scale),
        out_shape=(
            jax.ShapeDtypeStruct((part, hidden), F32),
            jax.ShapeDtypeStruct((2 * heads, hidden), F32),
        ),
        in_specs=[vmem] * 3
        + [pl.BlockSpec(memory_space=pl.ANY)]
        + [vmem] * 2
        + [pl.BlockSpec(memory_space=pltpu.SMEM)] * 3,
        out_specs=(vmem, vmem),
        scratch_shapes=[
            pltpu.VMEM((feat, hidden), BF16),
            pltpu.VMEM((n, rows, head), BF16),
            pltpu.VMEM((n, rows, head), BF16),
            pltpu.VMEM((total, head), BF16),
            pltpu.VMEM((total // 2, head), BF16),
            pltpu.VMEM((head, total // 2), BF16),
            pltpu.VMEM((chip_feat, total // 2), BF16),
            pltpu.VMEM((kd, rows), BF16),
            pltpu.VMEM((rows, hidden), F32),
            pltpu.VMEM((rows, hidden), BF16),
            pltpu.VMEM((2 * rows, total), F32),
            pltpu.VMEM((n, 8, rows), F32),
            pltpu.VMEM((2, chips, rows), F32),
            pltpu.VMEM((n, chips, rows), F32),
            pltpu.VMEM((chips, heads, rows), F32),
            pltpu.VMEM((chips, 2 * heads, rows), F32),
            pltpu.VMEM((total // 2, 2 * heads), BF16),
            pltpu.VMEM((CLASSES, total // 2, hidden // CLASSES), jnp.int16),
            pltpu.VMEM((CLASSES, total // 2, hidden // CLASSES), BF16),
            pltpu.VMEM((hidden // rows, 2 * heads, rows), F32),
            pltpu.VMEM((n, 2 * heads, rows), F32),
            pltpu.VMEM((2 * heads, rows), F32),
            pltpu.VMEM((nb - 1, 2 * heads, rows), F32),
            pltpu.VMEM((hidden // rows, 2 * heads, rows), F32),
            pltpu.VMEM((ROUNDS, chip_feat // 2, piece), F32),
            pltpu.VMEM((ROUNDS, chip_feat // 2, piece), F32),
            pltpu.VMEM((ROUNDS, grans + share_rows - 1, GRAN, piece), F32),
            pltpu.VMEM((ROUNDS, nb - 1, share_rows, GRAN, piece), F32),
            pltpu.VMEM((ROUNDS, share_rows, GRAN, piece), F32),
            pltpu.VMEM((ROUNDS, share_rows, GRAN, piece), F32),
            pltpu.SMEM((n,), jnp.int32),
            dma,
            dma((2,)),
            dma((2,)),
            dma((2,)),
            dma((2,)),
            dma((2,)),
            dma((2,)),
            dma((2,)),
            dma((CLASSES + 1, SIDE + 4)),
            dma((2,)),
            dma((2,)),
            dma((2,)),
            dma((2, ROUNDS)),
            dma((2, ROUNDS)),
            dma((2, share_rows)),
        ],
        compiler_params=pltpu.CompilerParams(
            collective_id=0, has_side_effects=True, vmem_limit_bytes=60 * 1024 * 1024
        ),
    )(
        q_rows,
        k_rows,
        v_rows,
        w_in,
        b_in[None, :],
        output_weight.T,
        output_bias[None, :],
        block_pos,
        lengths,
    )
    grad, gw, gb, ob = pl.pallas_call(
        emit,
        out_shape=(
            jax.ShapeDtypeStruct((part, hidden), F32),
            jax.ShapeDtypeStruct((heads, hidden), F32),
            jax.ShapeDtypeStruct((1, hidden), F32),
            jax.ShapeDtypeStruct((1, heads), F32),
        ),
        in_specs=[vmem] * 2,
        out_specs=(vmem,) * 4,
    )(grad, small)
    return (grad, gb[0], gw.T, ob[0])


def solution(mesh):
    return jax.shard_map(
        on_device,
        mesh=mesh,
        in_specs=(
            P("batch", "seq", None),
            P("batch", "seq", None),
            P("batch", "seq", None),
            P("batch"),
            P("batch", None),
            P(),
            P(),
            P(),
            P(),
        ),
        out_specs=(P(("seq", "batch"), None), P(), P(), P()),
        check_vma=False,
    )
```
